256 devices in a mesh: blk: 16 (over x, z_hi), slab: 16 (over y, z_lo, core).
Axes of the slice: x: 4, y: 4, z: 8 (z_hi: 4, z_lo: 2; z = z_hi * 2 + z_lo), core: 2. Of those that a mesh axis runs over, the one named last changes fastest.
Arguments:
- xinv: bfloat16 [16, 4096, 4096], P('blk', None, 'slab'), may hold values from -1 to 16
- ymat: bfloat16 [16, 4096, 4096], P('blk', None, 'slab'), may hold values from -1 to 16
- basis: bfloat16 [16, 4096, 1024], P('blk', 'slab'), may hold values from -0.08118988 to 0.08118988
- pair_index: int32 [16, 2, 512], P('blk'), may hold values from 0 to 1023
- orders: int32 [16], replicated, may hold values from 1 to 512, 4096 in all
- dest: int32 [16], replicated, may hold values from 0 to 15, each once
Outputs:
- factor: float32 [16, 512, 512], P('blk', 'slab')
The draws below stay inside these ranges and needn't reach their ends.
Inputs may be any that keep to these rules, and one draw needn't show every extreme that they name: `pair_index`: entries name columns of the block's basis. Sum of all orders is 4096; the largest equals 512. `dest`: every group receives exactly one block.
All inputs are finite; a program needn't handle non-finite values.
Results may differ from the reference program's by a relative error of at most 0.0003.
Values may be sent and summed in bfloat16 or wider, within the bound.
A program may use at most 64 MiB of HBM per device.

```python
import math
import jax
import jax.numpy as jnp
import numpy as np
from jax import lax

P_SIZE = 4096
R = 1024
MMAX = 512
BLOCKS = 16


shared_rank = 16


def positive_blocks(key):
    key_off, key_diag = jax.random.split(key, 2)
    noise = jax.random.normal(key_off, (BLOCKS, P_SIZE, P_SIZE), jnp.float32) * (0.2 / (2.0 * P_SIZE) ** 0.5)
    sym = noise + jnp.swapaxes(noise, 1, 2)
    diag = jnp.exp(jax.random.uniform(key_diag, (BLOCKS, P_SIZE), jnp.float32, 0.0, 1.386))
    eye = (jnp.arange(P_SIZE)[:, None] == jnp.arange(P_SIZE)[None, :]).astype(jnp.float32)
    whole = sym + eye[None] * diag[:, :, None]
    return whole


def draw_xinv(key, part):
    return positive_blocks(jax.random.fold_in(key, 11)).astype(jnp.bfloat16)


def draw_ymat(key, part):
    return positive_blocks(jax.random.fold_in(key, 23)).astype(jnp.bfloat16)


def draw_basis(key, part):
    key_noise, key_left, key_mix = jax.random.split(jax.random.fold_in(key, 37), 3)
    spread = 1.0 / P_SIZE ** 0.5
    shared_left = jax.random.normal(key_left, (BLOCKS, P_SIZE, shared_rank), jnp.float32) * spread
    shared_mix = jax.random.normal(key_mix, (BLOCKS, shared_rank, R), jnp.float32) * 0.34
    shared_part = jnp.einsum('bpk,bkr->bpr', shared_left, shared_mix, precision=lax.Precision.HIGHEST)
    own_part = jax.random.normal(key_noise, (BLOCKS, P_SIZE, R), jnp.float32) * spread
    whole = own_part + shared_part
    largest = (27.0 / P_SIZE) ** 0.5
    return jnp.clip(whole, -largest, largest).astype(jnp.bfloat16)


def with_ends(entries, stream_key, low, high):
    place = [jax.random.randint(jax.random.fold_in(stream_key, axis), (), 0, length) for axis, length in enumerate(entries.shape)]
    main_axis = entries.shape.index(max(entries.shape))
    next_to = place[:main_axis] + [(place[main_axis] + 1) % entries.shape[main_axis]] + place[main_axis + 1:]
    return entries.at[tuple(place)].set(low).at[tuple(next_to)].set(high)


def profile(count, total, reach, lean):
    weights = [(1 << 20) // math.isqrt(grade ** lean) + 1 for grade in range(2, count + 1)]
    spare, counts = total - reach - (count - 1), [1] * (count - 1)
    while spare > 0:
        free = [i for i in range(count - 1) if counts[i] < reach]
        whole, budget = sum([weights[i] for i in free]), spare
        for i in free:
            more = min(reach - counts[i], max(1, budget * weights[i] // whole), spare)
            counts[i] = counts[i] + more
            spare = spare - more
    return np.array([reach] + counts)


def ragged_sizes(rng, amount, total, reach, slope):
    if amount == 2:
        one = jax.random.randint(rng, (), max(1, total - reach), min(reach, total - 1) + 1)
        return jnp.stack([one, total - one])
    lengths = jnp.asarray(profile(amount, total, reach, slope), jnp.int32)
    twos = (amount - 1) // 2
    source_of, taker = lengths[1:1 + 2 * twos:2], lengths[2:2 + 2 * twos:2]
    slack = jnp.minimum(source_of - 1, reach - taker)
    shifted = jax.random.randint(jax.random.fold_in(rng, 1), (twos,), 0, 1 << 20) % (slack + 1)
    lengths = lengths.at[1:1 + 2 * twos:2].set(source_of - shifted).at[2:2 + 2 * twos:2].set(taker + shifted)
    return lengths[jax.random.permutation(jax.random.fold_in(rng, 2), amount)]


def setup_inputs(seed: int = 0) -> dict:
    streams_of = jax.random.split(jax.random.key(seed), 7)
    xinv = draw_xinv(jax.random.fold_in(streams_of[6], 71), 0)
    ymat = draw_ymat(jax.random.fold_in(streams_of[6], 71), 0)
    basis = draw_basis(jax.random.fold_in(streams_of[6], 71), 0)
    pair_index = with_ends(jax.random.randint(streams_of[3], (BLOCKS, 2, MMAX), 0, R), jax.random.fold_in(streams_of[3], 1), 0, R - 1).astype(jnp.int32)
    orders = ragged_sizes(streams_of[4], BLOCKS, BLOCKS * MMAX // 2, MMAX, 2).astype(jnp.int32)
    dest = jax.random.permutation(streams_of[5], BLOCKS).astype(jnp.int32)
    return {"xinv": xinv, "ymat": ymat, "basis": basis, "pair_index": pair_index, "orders": orders, "dest": dest}


def one_block(operands):
    xblock, yblock, vblock, index, order = operands
    vfloat = vblock.astype(jnp.float32)
    high = lax.Precision.HIGHEST
    cx = jnp.dot(vfloat.T, xblock.astype(jnp.float32), precision=high).astype(jnp.bfloat16)
    cy = jnp.dot(vfloat.T, yblock.astype(jnp.float32), precision=high).astype(jnp.bfloat16)
    cx = lax.optimization_barrier(cx)
    cy = lax.optimization_barrier(cy)
    apair = jnp.dot(cx.astype(jnp.float32), vfloat, precision=high)
    bpair = jnp.dot(cy.astype(jnp.float32), vfloat, precision=high)
    first = index[0]
    second = index[1]
    a_rows = apair[first]
    b_rows = bpair[second]
    schur = a_rows[:, first] * b_rows[:, second]
    live = jnp.arange(MMAX, dtype=jnp.int32) < order
    mask = live[:, None] & live[None, :]
    whole = jnp.where(mask, schur, 0.0) + jnp.eye(MMAX, dtype=jnp.float32)
    return jnp.linalg.cholesky(whole)

def reference(xinv, ymat, basis, pair_index, orders, dest):
    factors = lax.map(one_block, (xinv, ymat, basis, pair_index, orders))
    placed = jnp.zeros_like(factors).at[dest].set(factors)
    return placed
```

```python
import jax
import jax.numpy as jnp
from jax import lax
from jax.experimental import pallas as pl
from jax.experimental.pallas import tpu as pltpu
from jax.sharding import PartitionSpec as P

def lane_of(x, k):
    return jnp.broadcast_to(x[:, k:k + 1], x.shape)

def sub_of(x, k):
    return jnp.broadcast_to(x[k:k + 1, :], x.shape)

def panel(work, lo, p, lanes):
    wide = [lo + 128 * v for v in range(lanes)]
    top = lo + 8 * p
    rows = [work[pl.ds(top, 8), pl.ds(w, 128)] for w in wide]
    sub = lax.broadcasted_iota(jnp.int32, (8, 128), 0)
    cols = [lane_of(rows[0], 8 * p + b) for b in range(8)]
    scale = jnp.zeros((8, 128), jnp.float32)
    inv, coef, urow = [], [], []
    for k in range(8):
        r = lax.rsqrt(sub_of(cols[k], k))
        c = cols[k] * r
        cs = {b: sub_of(c, b) for b in range(k + 1, 8)}
        for b in range(k + 1, 8):
            cols[b] = cols[b] - c * cs[b]
        u = [sub_of(x, k) * r for x in rows]
        cm = jnp.where(sub > k, c, 0.0)
        rows = [x - cm * y for x, y in zip(rows, u)]
        scale = jnp.where(sub == k, r, scale)
        inv.append(r); coef.append(cs); urow.append(u)
    for x, w in zip(rows, wide):
        work[pl.ds(top, 8), pl.ds(w, 128)] = x * scale
    for g in range(p + 1, 16):
        at = lo + 8 * g
        rest = [work[pl.ds(at, 8), pl.ds(w, 128)] for w in wide]
        cols = [lane_of(rest[0], 8 * p + b) for b in range(8)]
        for k in range(8):
            c = cols[k] * inv[k]
            for b in range(k + 1, 8):
                cols[b] = cols[b] - c * coef[k][b]
            rest = [x - c * y for x, y in zip(rest, urow[k])]
        for x, w in zip(rest, wide):
            work[pl.ds(at, 8), pl.ds(w, 128)] = x

def factor(work, low, n):
    blocks = n // 128
    for j in range(blocks):
        lo = 128 * j
        for p in range(16):
            panel(work, lo, p, blocks - j)
        tri = lax.broadcasted_iota(jnp.int32, (128, 128), 0) >= lax.broadcasted_iota(jnp.int32, (128, 128), 1)
        low[pl.ds(lo, 128), pl.ds(lo, 128)] = jnp.where(tri, work[pl.ds(lo, 128), pl.ds(lo, 128)].T, 0.0)
        for i in range(j + 1, blocks):
            low[pl.ds(128 * i, 128), pl.ds(lo, 128)] = work[pl.ds(lo, 128), pl.ds(128 * i, 128)].T
            low[pl.ds(lo, 128), pl.ds(128 * i, 128)] = jnp.zeros((128, 128), jnp.float32)
        for i in range(j + 1, blocks):
            w = n - 128 * i
            work[pl.ds(128 * i, 128), pl.ds(128 * i, w)] = work[pl.ds(128 * i, 128), pl.ds(128 * i, w)] - lax.dot_general(
                low[pl.ds(128 * i, 128), pl.ds(lo, 128)], work[pl.ds(lo, 128), pl.ds(128 * i, w)],
                (((1,), (0,)), ((), ())), preferred_element_type=jnp.float32, precision=lax.Precision.HIGHEST)

def kernel(s_ref, l_ref, work):
    n = s_ref.shape[0]
    work[...] = s_ref[...]
    factor(work, l_ref, n)

def chol(s):
    n = s.shape[0]
    return pl.pallas_call(kernel, out_shape=jax.ShapeDtypeStruct((n, n), jnp.float32),
        in_specs=[pl.BlockSpec(memory_space=pltpu.VMEM)], out_specs=pl.BlockSpec(memory_space=pltpu.VMEM),
        scratch_shapes=[pltpu.VMEM((n, n), jnp.float32)])(s)


def cut_along(value, dim, length):
    before, after = (value.shape[:dim], value.shape[dim + 1 :])
    return jnp.moveaxis(value.reshape(*before, length, -1, *after), dim, 0)


def sum_at_owner(value, axis, dim):
    parts = cut_along(value, dim, lax.axis_size(axis))
    arrived = lax.all_to_all(parts, axis, split_axis=0, concat_axis=0, tiled=True)
    return arrived.sum(axis=0)


def from_everyone(value, axis):
    copies = jnp.broadcast_to(value, (lax.axis_size(axis), *value.shape))
    return lax.all_to_all(copies, axis, split_axis=0, concat_axis=0, tiled=True)


def in_order(parts, dim):
    parts = jnp.moveaxis(parts, 0, dim)
    lengths = parts.shape
    return parts.reshape(*lengths[:dim], lengths[dim] * lengths[dim + 1], *lengths[dim + 2 :])


def gathered_copies(value, axis, dim):
    parts = from_everyone(value, axis)
    return in_order(parts, dim)


def add_piece(piece, columns):
    return lax.dot_general(
        piece, columns, (((0,), (0,)), ((), ())), preferred_element_type=jnp.float32
    )


def on_device(xinv, ymat, basis, pair_index, orders, dest):
    xlocal = xinv[0]
    ylocal = ymat[0]
    vlocal = basis[0]
    piece = lax.all_gather(vlocal, "slab", axis=0, tiled=True)
    cx = add_piece(piece, xlocal)
    cy = add_piece(piece, ylocal)
    cx = cx.astype(jnp.bfloat16)
    cy = cy.astype(jnp.bfloat16)
    first = pair_index[0, 0]
    second = pair_index[0, 1]
    order_most = first.shape[0]
    share = order_most // lax.axis_size("slab")
    row_start = lax.axis_index("slab") * share
    basis_first = jnp.take(vlocal, first, axis=1)
    basis_second = jnp.take(vlocal, second, axis=1)
    cx_first = jnp.take(cx, first, axis=0)
    cy_second = jnp.take(cy, second, axis=0)
    stacked = sum_at_owner(
        jnp.concatenate(
            [
                jnp.dot(cx_first, basis_first, preferred_element_type=jnp.float32),
                jnp.dot(cy_second, basis_second, preferred_element_type=jnp.float32),
            ],
            axis=1,
        ),
        "slab",
        0,
    )
    a_ff = stacked[:, :order_most]
    b_ss = stacked[:, order_most:]
    schur = a_ff * b_ss
    block_id = lax.axis_index("blk")
    order = orders[block_id]
    row_ids = row_start + jnp.arange(share, dtype=jnp.int32)
    col_ids = jnp.arange(order_most, dtype=jnp.int32)
    mask = (row_ids[:, None] < order) & (col_ids[None, :] < order)
    diagonal = (row_ids[:, None] == col_ids[None, :]).astype(jnp.float32)
    schur_rows = jnp.where(mask, schur, 0.0) + diagonal
    everyone = gathered_copies(schur_rows, "blk", 0)
    groups = dest.shape[0]
    everyone = everyone.reshape(groups, share, order_most)
    chosen = (dest == block_id).astype(jnp.float32)
    mine = jnp.sum(chosen[:, None, None] * everyone, axis=0)
    whole = gathered_copies(mine, "slab", 0)
    lower = chol(whole)
    own = lax.dynamic_slice_in_dim(lower, row_start, share, 0)
    return own[None]


def solution(mesh):
    return jax.shard_map(
        on_device,
        mesh=mesh,
        in_specs=(
            P("blk", None, "slab"),
            P("blk", None, "slab"),
            P("blk", "slab", None),
            P("blk", None, None),
            P(),
            P(),
        ),
        out_specs=P("blk", "slab", None),
        check_vma=False,
    )
```

```python
import jax
import jax.numpy as jnp
from jax import lax
from jax.experimental import pallas as pl
from jax.experimental.pallas import tpu as pltpu
from jax.sharding import PartitionSpec as P

MESH = pl.DeviceIdType.MESH
CHUNKS = 4
ROWS, RANK, ORDER, FOLD = 256, 1024, 512, 640
PIECE = ROWS // CHUNKS
NT = (((1,), (1,)), ((), ()))
NN = (((1,), (0,)), ((), ()))


def mm(a, b, dims):
    return lax.dot_general(a, b, dims, preferred_element_type=jnp.float32)


def folded(i):
    a = i // 8
    cut = ORDER - 128 * a
    return ((16 * i, 128 * a, 0, cut), (16 * (31 - i), 128 * (3 - a), cut, FOLD - cut))


def pair_kernel(x_hbm, y_hbm, own, index, orders, s_ref, xin, xyt, held, passing, total, pick, turned,
                part, half, mine, came, pieces, load_sem, own_sem, far_sem, near_sem, sum_sem, out_sem):
    me = lax.axis_index("slab")
    y, z, k = lax.div(me, 4), lax.rem(lax.div(me, 2), 2), lax.rem(me, 2)
    chip = 2 * y + z
    up, down, across = lax.rem(y + 1, 4), lax.rem(y + 3, 4), 1 - z

    def at(yy, zz, kk):
        return {"slab": 4 * yy + 2 * zz + kk}

    sibling, beside = at(y, z, 1 - k), at(y, across, k)
    above, below = at(up, z, k), at(down, z, k)
    others = [(dy, dz) for dy in range(4) for dz in range(2) if (dy, dz) != (0, 0)]

    def chip_at(dy, dz):
        return lax.rem(y + dy, 4), z + dz - 2 * z * dz

    def send(src, dst, sems, i, to):
        return pltpu.make_async_remote_copy(
            src_ref=src, dst_ref=dst, send_sem=sems.at[0, i], recv_sem=sems.at[1, i],
            device_id=to, device_id_type=MESH)

    w = jnp.where(y >= 2, z, across)
    groups = (chip, 2 * y + across, 2 * down + z, 2 * down + across, 2 * lax.rem(y + 2, 4) + w)
    loads = []
    for m, src in enumerate((x_hbm, y_hbm)):
        for g, c in enumerate(groups):
            copy = pltpu.make_async_copy(
                src.at[pl.ds(pl.multiple_of(512 * c, 512), 512), :], xin.at[m, g], load_sem.at[5 * m + g])
            copy.start()
            loads.append(copy)

    barrier = pltpu.get_barrier_semaphore()
    pl.semaphore_signal(barrier, inc=1, device_id=sibling, device_id_type=MESH)
    for dy, dz in others:
        yy, zz = chip_at(dy, dz)
        pl.semaphore_signal(barrier, inc=1, device_id=at(yy, zz, k), device_id_type=MESH)
    pl.semaphore_wait(barrier, 8)

    base = pl.multiple_of(ROWS * k, ROWS)

    def rows(c):
        return pl.ds(pl.multiple_of(base + PIECE * c, PIECE), PIECE)

    def bit(c):
        return pl.ds(PIECE * c, PIECE)

    own_copy = send(own, held.at[0, pl.ds(base, ROWS), :], own_sem, 0, sibling)
    own_copy.start()
    z_copy = [send(own.at[bit(c), :], held.at[1, rows(c), :], far_sem, c, beside) for c in range(CHUNKS)]
    u_copy = [send(own.at[bit(c), :], held.at[2, rows(c), :], far_sem, CHUNKS + c, above) for c in range(CHUNKS)]
    w_copy = [send(held.at[1, rows(c), :], held.at[3, rows(c), :], far_sem, 2 * CHUNKS + c, above)
              for c in range(CHUNKS)]
    p_own = [send(own.at[bit(c), :], passing.at[bit(c), :], far_sem, 3 * CHUNKS + c, below) for c in range(CHUNKS)]
    p_held = [send(held.at[1, rows(c), :], passing.at[bit(c), :], far_sem, 3 * CHUNKS + c, below)
              for c in range(CHUNKS)]
    q_copy = [send(passing.at[bit(c), :], held.at[4, rows(c), :], far_sem, 4 * CHUNKS + c, below)
              for c in range(CHUNKS)]
    near = {g: [send(held.at[g, rows(c), :], held.at[g, rows(c), :], near_sem, CHUNKS * (g - 1) + c, sibling)
                for c in range(CHUNKS)] for g in (1, 2, 3, 4)}
    for c in range(CHUNKS):
        z_copy[c].start()
        u_copy[c].start()

    @pl.when(y < 2)
    def _():
        for c in range(CHUNKS):
            p_own[c].start()

    held[0, pl.ds(base, ROWS), :] = own[...]
    for m in range(2):
        wanted = jnp.broadcast_to(index[m:m + 1, :], (128, ORDER)).astype(jnp.float32).T
        for j in range(RANK // 128):
            lane = lax.broadcasted_iota(jnp.int32, (ORDER, 128), 1).astype(jnp.float32) + 128.0 * j
            pick[m, :, 128 * j:128 * j + 128] = jnp.where(wanted == lane, 1.0, 0.0).astype(jnp.bfloat16)
        turned[m, :, 256:512] = mm(pick[m], own[...], NT).astype(jnp.bfloat16)
    for copy in loads:
        copy.wait()
    for m in range(2):
        for g in range(5):
            xt = xin[m, g].T
            if g < 2:
                xt = xt * jnp.bfloat16(0.5)
            xyt[256 * m:256 * m + 256, 512 * g:512 * g + 512] = xt

    def gather_step(g, first=False):
        for j in range(RANK // 256):
            cols = slice(256 * j, 256 * j + 256)
            more = mm(xyt[:, 512 * g:512 * g + 512], held[g, :, cols], NN)
            total[:, cols] = more if first else total[:, cols] + more

    own_copy.wait_recv()
    gather_step(0, first=True)
    for c in range(CHUNKS):
        z_copy[c].wait_recv()
        w_copy[c].start()
        near[1][c].start()

        @pl.when(y >= 2)
        def _():
            p_held[c].start()

        p_own[c].wait_recv()
        q_copy[c].start()
    for c in range(CHUNKS):
        u_copy[c].wait_recv()
        near[2][c].start()
    for g in (1, 2):
        for c in range(CHUNKS):
            near[g][c].wait_recv()
        gather_step(g)
    for c in range(CHUNKS):
        w_copy[c].wait_recv()
        near[3][c].start()
        q_copy[c].wait_recv()
        near[4][c].start()
    for g in (3, 4):
        for c in range(CHUNKS):
            near[g][c].wait_recv()
        gather_step(g)

    half_copy = []
    for m in range(2):
        cxt = total[256 * m:256 * m + 256, :].astype(jnp.bfloat16)
        turned[m, :, 0:256] = mm(pick[m], cxt, NT).astype(jnp.bfloat16)
        for j in range(4):
            lo = 128 * j
            block = (mm(turned[m, lo:lo + 128, 0:256], turned[m, lo:, 256:512], NT)
                     + mm(turned[m, lo:lo + 128, 256:512], turned[m, lo:, 0:256], NT))
            for i in range(16):
                for row, col, lane, width in folded(i):
                    if lo <= row < lo + 128:
                        part[m, i % 2, i // 2, :, lane:lane + width] = block[row - lo:row - lo + 16, col - lo:]
        copy = send(part.at[m, 1 - k], half.at[m], sum_sem, m, sibling)
        copy.start()
        half_copy.append(copy)
    for m in range(2):
        half_copy[m].wait_recv()
        mine[:, :, FOLD * m:FOLD * m + FOLD] = part[m, k] + half[m]
    sums = []
    for n, (dy, dz) in enumerate(others):
        yy, zz = chip_at(dy, dz)
        copy = send(mine.at[2 * yy + zz], came.at[n], sum_sem, 2 + n, at(yy, zz, k))
        copy.start()
        sums.append(copy)
    both = mine[chip]
    for n in range(7):
        sums[n].wait_recv()
        both = both + came[n]

    lane = lax.broadcasted_iota(jnp.int32, (16, FOLD), 1)
    line = lax.broadcasted_iota(jnp.int32, (16, FOLD), 0)
    a = lax.div(me, 8)
    cut = ORDER - 128 * a
    low_part = lane < cut
    row = jnp.where(low_part, 16 * me, 16 * (31 - me)) + line
    col = jnp.where(low_part, 128 * a + lane, 128 * (3 - a) + lane - cut)
    order = orders[lax.axis_index("blk")]
    live = (row < order) & (col < order)
    pieces[me] = jnp.where(live, both[:, :FOLD] * both[:, FOLD:], 0.0) + jnp.where(row == col, 1.0, 0.0)

    outs = [send(pieces.at[me], pieces.at[me], out_sem, 0, sibling)]
    for n, (dy, dz) in enumerate(others):
        yy, zz = chip_at(dy, dz)
        outs.append(send(pieces.at[me], pieces.at[me], out_sem, 1 + n, at(yy, zz, k)))
    for copy in outs:
        copy.start()
    passed = []
    for n, (dy, dz) in enumerate(others):
        yy, zz = chip_at(4 - dy, dz)
        source = 4 * yy + 2 * zz + k
        outs[1 + n].wait_recv()
        copy = send(pieces.at[source], pieces.at[source], out_sem, 8 + n, sibling)
        copy.start()
        passed.append(copy)
    outs[0].wait_recv()
    for copy in passed:
        copy.wait_recv()
    for i in range(16):
        for row, col, lane, width in folded(i):
            s_ref[row:row + 16, col:col + width] = pieces[i, :, lane:lane + width]

    own_copy.wait_send()
    for copies in (z_copy, u_copy, w_copy, p_own, q_copy, near[1], near[2], near[3], near[4], half_copy, sums,
                   outs, passed):
        for copy in copies:
            copy.wait_send()


def schur_rows(x, y, v, index, orders):
    bf, f32 = jnp.bfloat16, jnp.float32
    vm, dma = pltpu.VMEM, pltpu.SemaphoreType.DMA
    return pl.pallas_call(
        pair_kernel,
        out_shape=jax.ShapeDtypeStruct((ORDER, ORDER), f32),
        in_specs=[pl.BlockSpec(memory_space=pl.ANY)] * 2 + [pl.BlockSpec(memory_space=vm)] * 2
        + [pl.BlockSpec(memory_space=pltpu.SMEM)],
        out_specs=pl.BlockSpec(memory_space=vm),
        scratch_shapes=[
            vm((2, 5, 512, 256), bf), vm((512, 2560), bf), vm((5, 512, RANK), bf), vm((ROWS, RANK), bf),
            vm((512, RANK), f32), vm((2, ORDER, RANK), bf), vm((2, ORDER, 512), bf),
            vm((2, 2, 8, 16, FOLD), f32), vm((2, 8, 16, FOLD), f32), vm((8, 16, 2 * FOLD), f32),
            vm((7, 16, 2 * FOLD), f32), vm((16, 16, FOLD), f32),
            dma((10,)), dma((2, 1)), dma((2, 5 * CHUNKS)), dma((2, 4 * CHUNKS)), dma((2, 9)), dma((2, 15)),
        ],
        compiler_params=pltpu.CompilerParams(collective_id=0, has_side_effects=True),
    )(x, y, v, index, orders)


def lane_of(x, k):
    return jnp.broadcast_to(x[:, k:k + 1], x.shape)


def sub_of(x, k):
    return jnp.broadcast_to(x[k:k + 1, :], x.shape)


def panel(work, lo, p, lanes):
    wide = [lo + 128 * v for v in range(lanes)]
    top = lo + 8 * p
    rows = [work[pl.ds(top, 8), pl.ds(w, 128)] for w in wide]
    sub = lax.broadcasted_iota(jnp.int32, (8, 128), 0)
    cols = [lane_of(rows[0], 8 * p + b) for b in range(8)]
    scale = jnp.zeros((8, 128), jnp.float32)
    inv, coef, urow = [], [], []
    for k in range(8):
        r = lax.rsqrt(sub_of(cols[k], k))
        c = cols[k] * r
        cs = {b: sub_of(c, b) for b in range(k + 1, 8)}
        for b in range(k + 1, 8):
            cols[b] = cols[b] - c * cs[b]
        u = [sub_of(x, k) * r for x in rows]
        cm = jnp.where(sub > k, c, 0.0)
        rows = [x - cm * y for x, y in zip(rows, u)]
        scale = jnp.where(sub == k, r, scale)
        inv.append(r); coef.append(cs); urow.append(u)
    for x, w in zip(rows, wide):
        work[pl.ds(top, 8), pl.ds(w, 128)] = x * scale
    for g in range(p + 1, 16):
        at = lo + 8 * g
        rest = [work[pl.ds(at, 8), pl.ds(w, 128)] for w in wide]
        cols = [lane_of(rest[0], 8 * p + b) for b in range(8)]
        for k in range(8):
            c = cols[k] * inv[k]
            for b in range(k + 1, 8):
                cols[b] = cols[b] - c * coef[k][b]
            rest = [x - c * y for x, y in zip(rest, urow[k])]
        for x, w in zip(rest, wide):
            work[pl.ds(at, 8), pl.ds(w, 128)] = x


def factor(work, low, n):
    blocks = n // 128
    for j in range(blocks):
        lo = 128 * j
        for p in range(16):
            panel(work, lo, p, blocks - j)
        tri = lax.broadcasted_iota(jnp.int32, (128, 128), 0) >= lax.broadcasted_iota(jnp.int32, (128, 128), 1)
        low[pl.ds(lo, 128), pl.ds(lo, 128)] = jnp.where(tri, work[pl.ds(lo, 128), pl.ds(lo, 128)].T, 0.0)
        for i in range(j + 1, blocks):
            low[pl.ds(128 * i, 128), pl.ds(lo, 128)] = work[pl.ds(lo, 128), pl.ds(128 * i, 128)].T
            low[pl.ds(lo, 128), pl.ds(128 * i, 128)] = jnp.zeros((128, 128), jnp.float32)
        for i in range(j + 1, blocks):
            w = n - 128 * i
            work[pl.ds(128 * i, 128), pl.ds(128 * i, w)] = work[pl.ds(128 * i, 128), pl.ds(128 * i, w)] - lax.dot_general(
                low[pl.ds(128 * i, 128), pl.ds(lo, 128)], work[pl.ds(lo, 128), pl.ds(128 * i, w)],
                (((1,), (0,)), ((), ())), preferred_element_type=jnp.float32, precision=lax.Precision.HIGHEST)


def chol_kernel(s_ref, own_ref, work, low):
    n, share = s_ref.shape[0], own_ref.shape[0]
    work[...] = s_ref[...]
    factor(work, low, n)
    own_ref[...] = low[pl.ds(pl.multiple_of(share * lax.axis_index("slab"), share), share), :]


def chol_rows(s, share):
    n = s.shape[0]
    return pl.pallas_call(
        chol_kernel,
        out_shape=jax.ShapeDtypeStruct((share, n), jnp.float32),
        in_specs=[pl.BlockSpec(memory_space=pltpu.VMEM)],
        out_specs=pl.BlockSpec(memory_space=pltpu.VMEM),
        scratch_shapes=[pltpu.VMEM((n, n), jnp.float32)] * 2,
    )(s)


def route_kernel(l_ref, dest, out_ref, along, sent, came, x_sem, z_sem):
    me = lax.axis_index("blk")
    x, h = lax.div(me, 4), lax.rem(me, 4)

    def send(src, dst, sems, i, to):
        return pltpu.make_async_remote_copy(
            src_ref=src, dst_ref=dst, send_sem=sems.at[0, i], recv_sem=sems.at[1, i],
            device_id={"blk": to}, device_id_type=MESH)

    def x_at(d):
        return 4 * lax.rem(x + d, 4) + h

    def h_at(d):
        return 4 * x + lax.rem(h + d, 4)

    barrier = pltpu.get_barrier_semaphore()
    for d in (1, 2, 3):
        for to in (x_at(d), h_at(d)):
            pl.semaphore_signal(barrier, inc=1, device_id={"blk": to}, device_id_type=MESH)
    pl.semaphore_wait(barrier, 6)
    first = [send(l_ref, along.at[d - 1], x_sem, d - 1, x_at(d)) for d in (1, 2, 3)]
    for copy in first:
        copy.start()
    have = [(me, l_ref[...])]
    for d in (1, 2, 3):
        first[d - 1].wait_recv()
        have.append((x_at(4 - d), along[d - 1]))

    def bound_for(to):
        kept = jnp.zeros(l_ref.shape, jnp.float32)
        for block, value in have:
            kept = jnp.where(dest[block] == to, value, kept)
        return kept

    second = []
    for d in (2, 1, 3):
        sent[d - 1] = bound_for(h_at(d))
        copy = send(sent.at[d - 1], came.at[d - 1], z_sem, d - 1, h_at(d))
        copy.start()
        second.append((d, copy))
    result = bound_for(me)
    for d, copy in second:
        copy.wait_recv()
        result = result + came[d - 1]
    out_ref[0] = result
    for copy in first + [c for _, c in second]:
        copy.wait_send()


def route(rows, dest):
    vm, dma = pltpu.VMEM, pltpu.SemaphoreType.DMA
    return pl.pallas_call(
        route_kernel,
        out_shape=jax.ShapeDtypeStruct((1, *rows.shape), jnp.float32),
        in_specs=[pl.BlockSpec(memory_space=vm), pl.BlockSpec(memory_space=pltpu.SMEM)],
        out_specs=pl.BlockSpec(memory_space=vm),
        scratch_shapes=[vm((3, *rows.shape), jnp.float32)] * 3 + [dma((2, 3)), dma((2, 3))],
        compiler_params=pltpu.CompilerParams(collective_id=1, has_side_effects=True),
    )(rows, dest)


def on_device(xinv, ymat, basis, pair_index, orders, dest):
    whole = schur_rows(xinv[0], ymat[0], basis[0], pair_index[0], orders)
    rows = chol_rows(whole, ORDER // lax.axis_size("slab"))
    return route(rows, dest)


def solution(mesh):
    return jax.shard_map(
        on_device,
        mesh=mesh,
        in_specs=(
            P("blk", None, "slab"),
            P("blk", None, "slab"),
            P("blk", "slab", None),
            P("blk", None, None),
            P(),
            P(),
        ),
        out_specs=P("blk", "slab", None),
        check_vma=False,
    )
```

```python
import jax
import jax.numpy as jnp
from jax import lax
from jax.experimental import pallas as pl
from jax.experimental.pallas import tpu as pltpu
from jax.sharding import PartitionSpec as P

MESH = pl.DeviceIdType.MESH
CHUNKS = 4
ROWS, RANK, ORDER, FOLD = 256, 1024, 512, 640
PIECE = ROWS // CHUNKS
NT = (((1,), (1,)), ((), ()))
NN = (((1,), (0,)), ((), ()))


def mm(a, b, dims):
    return lax.dot_general(a, b, dims, preferred_element_type=jnp.float32)


def folded(i):
    a = i // 8
    cut = ORDER - 128 * a
    return ((16 * i, 128 * a, 0, cut), (16 * (31 - i), 128 * (3 - a), cut, FOLD - cut))


def pair_kernel(x_hbm, y_hbm, own, index, orders, dest, s_ref, xin, xyt, held, total, pick, turned,
                part, half, mine, came, formed, along, bound, brought, pieces,
                load_sem, own_sem, far_sem, near_sem, sum_sem, x_sem, h_sem, out_sem):
    me = lax.axis_index("slab")
    y, z, k = lax.div(me, 4), lax.rem(lax.div(me, 2), 2), lax.rem(me, 2)
    chip = 2 * y + z
    group = lax.axis_index("blk")
    bx, bh = lax.div(group, 4), lax.rem(group, 4)
    up, down, across = lax.rem(y + 1, 4), lax.rem(y + 3, 4), 1 - z

    def at(yy, zz, kk):
        return {"slab": 4 * yy + 2 * zz + kk}

    sibling, beside = at(y, z, 1 - k), at(y, across, k)
    above, below, slant = at(up, z, k), at(down, z, k), at(down, across, k)
    opposite = at(lax.rem(y + 2, 4), z, k)
    others = [(dy, dz) for dy in range(4) for dz in range(2) if (dy, dz) != (0, 0)]

    def chip_at(dy, dz):
        return lax.rem(y + dy, 4), z + dz - 2 * z * dz

    def send(src, dst, sems, i, to):
        return pltpu.make_async_remote_copy(
            src_ref=src, dst_ref=dst, send_sem=sems.at[0, i], recv_sem=sems.at[1, i],
            device_id=to, device_id_type=MESH)

    def x_at(d):
        return 4 * lax.rem(bx + d, 4) + bh

    def h_at(d):
        return 4 * bx + lax.rem(bh + d, 4)

    w = jnp.where(y >= 2, z, across)
    groups = (chip, 2 * y + across, 2 * down + z, 2 * up + across, 2 * lax.rem(y + 2, 4) + w)
    loads = []
    for m, src in enumerate((x_hbm, y_hbm)):
        for g, c in enumerate(groups):
            copy = pltpu.make_async_copy(
                src.at[pl.ds(pl.multiple_of(512 * c, 512), 512), :], xin.at[m, g], load_sem.at[5 * m + g])
            copy.start()
            loads.append(copy)

    barrier = pltpu.get_barrier_semaphore()
    pl.semaphore_signal(barrier, inc=1, device_id=sibling, device_id_type=MESH)
    for dy, dz in others:
        yy, zz = chip_at(dy, dz)
        pl.semaphore_signal(barrier, inc=1, device_id=at(yy, zz, k), device_id_type=MESH)
    for d in (1, 2, 3):
        for to in (x_at(d), h_at(d)):
            pl.semaphore_signal(barrier, inc=1, device_id={"blk": to}, device_id_type=MESH)
    pl.semaphore_wait(barrier, 14)

    base = pl.multiple_of(ROWS * k, ROWS)

    def rows(c):
        return pl.ds(pl.multiple_of(base + PIECE * c, PIECE), PIECE)

    def bit(c):
        return pl.ds(PIECE * c, PIECE)

    own_copy = send(own, held.at[0, pl.ds(base, ROWS), :], own_sem, 0, sibling)
    own_copy.start()
    z_copy = [send(own.at[bit(c), :], held.at[1, rows(c), :], far_sem, c, beside) for c in range(CHUNKS)]
    u_copy = [send(own.at[bit(c), :], held.at[2, rows(c), :], far_sem, CHUNKS + c, above) for c in range(CHUNKS)]
    w_copy = [send(held.at[1, rows(c), :] if c < CHUNKS // 2 else own.at[bit(c), :], held.at[3, rows(c), :],
                   far_sem, 2 * CHUNKS + c, below if c < CHUNKS // 2 else slant) for c in range(CHUNKS)]
    p_own = [send(own.at[bit(c), :], held.at[4, rows(c), :], far_sem, 3 * CHUNKS + c, opposite)
             for c in range(CHUNKS)]
    p_held = [send(held.at[1, rows(c), :], held.at[4, rows(c), :], far_sem, 3 * CHUNKS + c, opposite)
              for c in range(CHUNKS)]
    near = {g: [send(held.at[g, rows(c), :], held.at[g, rows(c), :], near_sem, CHUNKS * (g - 1) + c, sibling)
                for c in range(CHUNKS)] for g in (1, 2, 3, 4)}
    for c in range(CHUNKS):
        z_copy[c].start()
        u_copy[c].start()
    for c in range(CHUNKS // 2, CHUNKS):
        w_copy[c].start()

    @pl.when(y < 2)
    def _():
        for c in range(CHUNKS):
            p_own[c].start()

    held[0, pl.ds(base, ROWS), :] = own[...]
    for m in range(2):
        wanted = jnp.broadcast_to(index[m:m + 1, :], (128, ORDER)).astype(jnp.float32).T
        for j in range(RANK // 128):
            lane = lax.broadcasted_iota(jnp.int32, (ORDER, 128), 1).astype(jnp.float32) + 128.0 * j
            pick[m, :, 128 * j:128 * j + 128] = jnp.where(wanted == lane, 1.0, 0.0).astype(jnp.bfloat16)
        turned[m, :, 256:512] = mm(pick[m], own[...], NT).astype(jnp.bfloat16)
    for copy in loads:
        copy.wait()
    for m in range(2):
        for g in range(5):
            xt = xin[m, g].T
            if g < 2:
                xt = xt * jnp.bfloat16(0.5)
            xyt[256 * m:256 * m + 256, 512 * g:512 * g + 512] = xt

    def gather_step(g, first=False):
        for j in range(RANK // 256):
            cols = slice(256 * j, 256 * j + 256)
            more = mm(xyt[:, 512 * g:512 * g + 512], held[g, :, cols], NN)
            total[:, cols] = more if first else total[:, cols] + more

    own_copy.wait_recv()
    gather_step(0, first=True)
    for c in range(CHUNKS):
        z_copy[c].wait_recv()
        if c < CHUNKS // 2:
            w_copy[c].start()

        @pl.when(y >= 2)
        def _():
            p_held[c].start()

        near[1][c].start()
    for c in range(CHUNKS):
        near[1][c].wait_recv()
    gather_step(1)
    for c in range(CHUNKS):
        u_copy[c].wait_recv()
        near[2][c].start()
    for c in range(CHUNKS):
        near[2][c].wait_recv()
    gather_step(2)
    for c in range(CHUNKS):
        w_copy[c].wait_recv()
        near[3][c].start()
        p_own[c].wait_recv()
        near[4][c].start()
    for g in (3, 4):
        for c in range(CHUNKS):
            near[g][c].wait_recv()
        gather_step(g)

    half_copy = []
    for m in range(2):
        cxt = total[256 * m:256 * m + 256, :].astype(jnp.bfloat16)
        turned[m, :, 0:256] = mm(pick[m], cxt, NT).astype(jnp.bfloat16)
        for j in range(4):
            lo = 128 * j
            block = (mm(turned[m, lo:lo + 128, 0:256], turned[m, lo:, 256:512], NT)
                     + mm(turned[m, lo:lo + 128, 256:512], turned[m, lo:, 0:256], NT))
            for i in range(16):
                for row, col, lane, width in folded(i):
                    if lo <= row < lo + 128:
                        part[m, i % 2, i // 2, :, lane:lane + width] = block[row - lo:row - lo + 16, col - lo:]
        copy = send(part.at[m, 1 - k], half.at[m], sum_sem, m, sibling)
        copy.start()
        half_copy.append(copy)
    sums = [[], []]
    for m in range(2):
        half_copy[m].wait_recv()
        mine[m] = part[m, k] + half[m]
        for n, (dy, dz) in enumerate(others):
            yy, zz = chip_at(dy, dz)
            copy = send(mine.at[m, 2 * yy + zz], came.at[m, n], sum_sem, 2 + 7 * m + n, at(yy, zz, k))
            copy.start()
            sums[m].append(copy)
    both = []
    for m in range(2):
        whole = mine[m, chip]
        for n in range(7):
            sums[m][n].wait_recv()
            whole = whole + came[m, n]
        both.append(whole)

    lane = lax.broadcasted_iota(jnp.int32, (16, FOLD), 1)
    line = lax.broadcasted_iota(jnp.int32, (16, FOLD), 0)
    a = lax.div(me, 8)
    cut = ORDER - 128 * a
    low_part = lane < cut
    row = jnp.where(low_part, 16 * me, 16 * (31 - me)) + line
    col = jnp.where(low_part, 128 * a + lane, 128 * (3 - a) + lane - cut)
    order = orders[group]
    live = (row < order) & (col < order)
    formed[...] = jnp.where(live, both[0] * both[1], 0.0) + jnp.where(row == col, 1.0, 0.0)

    first = [send(formed, along.at[d - 1], x_sem, d - 1, {"blk": x_at(d)}) for d in (1, 2, 3)]
    for copy in first:
        copy.start()
    have = [(group, formed[...])]
    for d in (1, 2, 3):
        first[d - 1].wait_recv()
        have.append((x_at(4 - d), along[d - 1]))

    def bound_for(to):
        kept = jnp.zeros((16, FOLD), jnp.float32)
        for source, value in have:
            kept = jnp.where(dest[source] == to, value, kept)
        return kept

    second = []
    for d in (2, 1, 3):
        bound[d - 1] = bound_for(h_at(d))
        copy = send(bound.at[d - 1], brought.at[d - 1], h_sem, d - 1, {"blk": h_at(d)})
        copy.start()
        second.append((d, copy))
    here = bound_for(group)
    for d, copy in second:
        copy.wait_recv()
        here = here + brought[d - 1]
    pieces[me] = here

    outs = [send(pieces.at[me], pieces.at[me], out_sem, 0, sibling)]
    for n, (dy, dz) in enumerate(others):
        yy, zz = chip_at(dy, dz)
        outs.append(send(pieces.at[me], pieces.at[me], out_sem, 1 + n, at(yy, zz, k)))
    for copy in outs:
        copy.start()
    passed = []
    for n, (dy, dz) in enumerate(others):
        yy, zz = chip_at(4 - dy, dz)
        source = 4 * yy + 2 * zz + k
        outs[1 + n].wait_recv()
        copy = send(pieces.at[source], pieces.at[source], out_sem, 8 + n, sibling)
        copy.start()
        passed.append(copy)
    outs[0].wait_recv()
    for copy in passed:
        copy.wait_recv()
    for i in range(16):
        for row, col, lane, width in folded(i):
            s_ref[row:row + 16, col:col + width] = pieces[i, :, lane:lane + width]

    own_copy.wait_send()
    for copies in (z_copy, u_copy, w_copy, p_own, near[1], near[2], near[3], near[4], half_copy, *sums, first,
                   [copy for _, copy in second], outs, passed):
        for copy in copies:
            copy.wait_send()


def schur_block(x, y, v, index, orders, dest):
    bf, f32 = jnp.bfloat16, jnp.float32
    vm, dma = pltpu.VMEM, pltpu.SemaphoreType.DMA
    return pl.pallas_call(
        pair_kernel,
        out_shape=jax.ShapeDtypeStruct((ORDER, ORDER), f32),
        in_specs=[pl.BlockSpec(memory_space=pl.ANY)] * 2 + [pl.BlockSpec(memory_space=vm)] * 2
        + [pl.BlockSpec(memory_space=pltpu.SMEM)] * 2,
        out_specs=pl.BlockSpec(memory_space=vm),
        scratch_shapes=[
            vm((2, 5, 512, 256), bf), vm((512, 2560), bf), vm((5, 512, RANK), bf),
            vm((512, RANK), f32), vm((2, ORDER, RANK), bf), vm((2, ORDER, 512), bf),
            vm((2, 2, 8, 16, FOLD), f32), vm((2, 8, 16, FOLD), f32), vm((2, 8, 16, FOLD), f32),
            vm((2, 7, 16, FOLD), f32), vm((16, FOLD), f32), vm((3, 16, FOLD), f32), vm((3, 16, FOLD), f32),
            vm((3, 16, FOLD), f32), vm((16, 16, FOLD), f32),
            dma((10,)), dma((2, 1)), dma((2, 4 * CHUNKS)), dma((2, 4 * CHUNKS)), dma((2, 16)),
            dma((2, 3)), dma((2, 3)), dma((2, 15)),
        ],
        compiler_params=pltpu.CompilerParams(collective_id=0, has_side_effects=True),
    )(x, y, v, index, orders, dest)


def lane_of(x, k):
    return jnp.broadcast_to(x[:, k:k + 1], x.shape)


def sub_of(x, k):
    return jnp.broadcast_to(x[k:k + 1, :], x.shape)


def panel(work, lo, p, lanes):
    wide = [lo + 128 * v for v in range(lanes)]
    top = lo + 8 * p
    rows = [work[pl.ds(top, 8), pl.ds(w, 128)] for w in wide]
    sub = lax.broadcasted_iota(jnp.int32, (8, 128), 0)
    cols = [lane_of(rows[0], 8 * p + b) for b in range(8)]
    scale = jnp.zeros((8, 128), jnp.float32)
    inv, coef, urow = [], [], []
    for k in range(8):
        r = lax.rsqrt(sub_of(cols[k], k))
        c = cols[k] * r
        cs = {b: sub_of(c, b) for b in range(k + 1, 8)}
        for b in range(k + 1, 8):
            cols[b] = cols[b] - c * cs[b]
        u = [sub_of(x, k) * r for x in rows]
        cm = jnp.where(sub > k, c, 0.0)
        rows = [x - cm * y for x, y in zip(rows, u)]
        scale = jnp.where(sub == k, r, scale)
        inv.append(r); coef.append(cs); urow.append(u)
    for x, w in zip(rows, wide):
        work[pl.ds(top, 8), pl.ds(w, 128)] = x * scale
    for g in range(p + 1, 16):
        at = lo + 8 * g
        rest = [work[pl.ds(at, 8), pl.ds(w, 128)] for w in wide]
        cols = [lane_of(rest[0], 8 * p + b) for b in range(8)]
        for k in range(8):
            c = cols[k] * inv[k]
            for b in range(k + 1, 8):
                cols[b] = cols[b] - c * coef[k][b]
            rest = [x - c * y for x, y in zip(rest, urow[k])]
        for x, w in zip(rest, wide):
            work[pl.ds(at, 8), pl.ds(w, 128)] = x


def factor(work, low, n):
    blocks = n // 128
    for j in range(blocks):
        lo = 128 * j
        for p in range(16):
            panel(work, lo, p, blocks - j)
        tri = lax.broadcasted_iota(jnp.int32, (128, 128), 0) >= lax.broadcasted_iota(jnp.int32, (128, 128), 1)
        low[pl.ds(lo, 128), pl.ds(lo, 128)] = jnp.where(tri, work[pl.ds(lo, 128), pl.ds(lo, 128)].T, 0.0)
        for i in range(j + 1, blocks):
            low[pl.ds(128 * i, 128), pl.ds(lo, 128)] = work[pl.ds(lo, 128), pl.ds(128 * i, 128)].T
            low[pl.ds(lo, 128), pl.ds(128 * i, 128)] = jnp.zeros((128, 128), jnp.float32)
        for i in range(j + 1, blocks):
            w = n - 128 * i
            work[pl.ds(128 * i, 128), pl.ds(128 * i, w)] = work[pl.ds(128 * i, 128), pl.ds(128 * i, w)] - lax.dot_general(
                low[pl.ds(128 * i, 128), pl.ds(lo, 128)], work[pl.ds(lo, 128), pl.ds(128 * i, w)],
                (((1,), (0,)), ((), ())), preferred_element_type=jnp.float32, precision=lax.Precision.HIGHEST)


def chol_kernel(s_ref, own_ref, work, low):
    n, share = s_ref.shape[0], own_ref.shape[0]
    work[...] = s_ref[...]
    factor(work, low, n)
    own_ref[...] = low[pl.ds(pl.multiple_of(share * lax.axis_index("slab"), share), share), :]


def chol_rows(s, share):
    n = s.shape[0]
    return pl.pallas_call(
        chol_kernel,
        out_shape=jax.ShapeDtypeStruct((share, n), jnp.float32),
        in_specs=[pl.BlockSpec(memory_space=pltpu.VMEM)],
        out_specs=pl.BlockSpec(memory_space=pltpu.VMEM),
        scratch_shapes=[pltpu.VMEM((n, n), jnp.float32)] * 2,
    )(s)


def on_device(xinv, ymat, basis, pair_index, orders, dest):
    whole = schur_block(xinv[0], ymat[0], basis[0], pair_index[0], orders, dest)
    return chol_rows(whole, ORDER // lax.axis_size("slab"))[None]


def solution(mesh):
    return jax.shard_map(
        on_device,
        mesh=mesh,
        in_specs=(
            P("blk", None, "slab"),
            P("blk", None, "slab"),
            P("blk", "slab", None),
            P("blk", None, None),
            P(),
            P(),
        ),
        out_specs=P("blk", "slab", None),
        check_vma=False,
    )
```

```python
import jax
import jax.numpy as jnp
from jax import lax
from jax.experimental import pallas as pl
from jax.experimental.pallas import tpu as pltpu
from jax.sharding import PartitionSpec as P

MESH = pl.DeviceIdType.MESH
CHUNKS = 4
ROWS, RANK, ORDER, FOLD = 256, 1024, 512, 640
PIECE = ROWS // CHUNKS
NT = (((1,), (1,)), ((), ()))
NN = (((1,), (0,)), ((), ()))


def mm(a, b, dims):
    return lax.dot_general(a, b, dims, preferred_element_type=jnp.float32)


def folded(i):
    a = i // 8
    cut = ORDER - 128 * a
    return ((16 * i, 128 * a, 0, cut), (16 * (31 - i), 128 * (3 - a), cut, FOLD - cut))


def pair_kernel(x_hbm, y_hbm, own, index, orders, dest, s_ref, xin, xyt, held, total, pick, turned,
                part, half, mine, came, formed, along, bound, brought, pieces,
                load_sem, own_sem, far_sem, near_sem, sum_sem, x_sem, h_sem, out_sem):
    me = lax.axis_index("slab")
    y, z, k = lax.div(me, 4), lax.rem(lax.div(me, 2), 2), lax.rem(me, 2)
    chip = 2 * y + z
    group = lax.axis_index("blk")
    bx, bh = lax.div(group, 4), lax.rem(group, 4)
    up, down, across = lax.rem(y + 1, 4), lax.rem(y + 3, 4), 1 - z

    def at(yy, zz, kk):
        return {"slab": 4 * yy + 2 * zz + kk}

    sibling, beside = at(y, z, 1 - k), at(y, across, k)
    above, below, slant = at(up, z, k), at(down, z, k), at(down, across, k)
    opposite = at(lax.rem(y + 2, 4), z, k)
    others = [(dy, dz) for dy in range(4) for dz in range(2) if (dy, dz) != (0, 0)]

    def chip_at(dy, dz):
        return lax.rem(y + dy, 4), z + dz - 2 * z * dz

    def send(src, dst, sems, i, to):
        return pltpu.make_async_remote_copy(
            src_ref=src, dst_ref=dst, send_sem=sems.at[0, i], recv_sem=sems.at[1, i],
            device_id=to, device_id_type=MESH)

    def x_at(d):
        return 4 * lax.rem(bx + d, 4) + bh

    def h_at(d):
        return 4 * bx + lax.rem(bh + d, 4)

    w = jnp.where(y >= 2, z, across)
    groups = (chip, 2 * y + across, 2 * down + z, 2 * up + across, 2 * lax.rem(y + 2, 4) + w)
    loads = []
    for m, src in enumerate((x_hbm, y_hbm)):
        for g, c in enumerate(groups):
            copy = pltpu.make_async_copy(
                src.at[pl.ds(pl.multiple_of(512 * c, 512), 512), :], xin.at[m, g], load_sem.at[5 * m + g])
            copy.start()
            loads.append(copy)

    barrier = pltpu.get_barrier_semaphore()
    pl.semaphore_signal(barrier, inc=1, device_id=sibling, device_id_type=MESH)
    for dy, dz in others:
        yy, zz = chip_at(dy, dz)
        pl.semaphore_signal(barrier, inc=1, device_id=at(yy, zz, k), device_id_type=MESH)
    for d in (1, 2, 3):
        for to in (x_at(d), h_at(d)):
            pl.semaphore_signal(barrier, inc=1, device_id={"blk": to}, device_id_type=MESH)
    pl.semaphore_wait(barrier, 14)

    base = pl.multiple_of(ROWS * k, ROWS)

    def rows(c):
        return pl.ds(pl.multiple_of(base + PIECE * c, PIECE), PIECE)

    def bit(c):
        return pl.ds(PIECE * c, PIECE)

    own_copy = send(own, held.at[0, pl.ds(base, ROWS), :], own_sem, 0, sibling)
    own_copy.start()
    z_copy = [send(own.at[bit(c), :], held.at[1, rows(c), :], far_sem, c, beside) for c in range(CHUNKS)]
    u_copy = [send(own.at[bit(c), :], held.at[2, rows(c), :], far_sem, CHUNKS + c, above) for c in range(CHUNKS)]
    w_copy = [send(held.at[1, rows(c), :] if c < CHUNKS // 2 else own.at[bit(c), :], held.at[3, rows(c), :],
                   far_sem, 2 * CHUNKS + c, below if c < CHUNKS // 2 else slant) for c in range(CHUNKS)]
    p_own = [send(own.at[bit(c), :], held.at[4, rows(c), :], far_sem, 3 * CHUNKS + c, opposite)
             for c in range(CHUNKS)]
    p_held = [send(held.at[1, rows(c), :], held.at[4, rows(c), :], far_sem, 3 * CHUNKS + c, opposite)
              for c in range(CHUNKS)]
    near = {g: [send(held.at[g, rows(c), :], held.at[g, rows(c), :], near_sem, CHUNKS * (g - 1) + c, sibling)
                for c in range(CHUNKS)] for g in (1, 2, 3, 4)}
    for c in range(CHUNKS):
        z_copy[c].start()
        u_copy[c].start()
    for c in range(CHUNKS // 2, CHUNKS):
        w_copy[c].start()

    @pl.when(y < 2)
    def _():
        for c in range(CHUNKS):
            p_own[c].start()

    held[0, pl.ds(base, ROWS), :] = own[...]
    for m in range(2):
        wanted = jnp.broadcast_to(index[m:m + 1, :], (128, ORDER)).astype(jnp.float32).T
        for j in range(RANK // 128):
            lane = lax.broadcasted_iota(jnp.int32, (ORDER, 128), 1).astype(jnp.float32) + 128.0 * j
            pick[m, :, 128 * j:128 * j + 128] = jnp.where(wanted == lane, 1.0, 0.0).astype(jnp.bfloat16)
        turned[m, :, 256:512] = mm(pick[m], own[...], NT).astype(jnp.bfloat16)
    for copy in loads:
        copy.wait()
    for m in range(2):
        for g in range(5):
            xt = xin[m, g].T
            if g < 2:
                xt = xt * jnp.bfloat16(0.5)
            xyt[256 * m:256 * m + 256, 512 * g:512 * g + 512] = xt

    def gather_step(g, first=False):
        for j in range(RANK // 256):
            cols = slice(256 * j, 256 * j + 256)
            more = mm(xyt[:, 512 * g:512 * g + 512], held[g, :, cols], NN)
            total[:, cols] = more if first else total[:, cols] + more

    own_copy.wait_recv()
    gather_step(0, first=True)
    for c in range(CHUNKS):
        z_copy[c].wait_recv()
        if c < CHUNKS // 2:
            w_copy[c].start()

        @pl.when(y >= 2)
        def _():
            p_held[c].start()

        near[1][c].start()
    for c in range(CHUNKS):
        near[1][c].wait_recv()
    gather_step(1)
    for c in range(CHUNKS):
        u_copy[c].wait_recv()
        near[2][c].start()
    for c in range(CHUNKS):
        near[2][c].wait_recv()
    gather_step(2)
    for c in range(CHUNKS):
        w_copy[c].wait_recv()
        near[3][c].start()
        p_own[c].wait_recv()
        near[4][c].start()
    for g in (3, 4):
        for c in range(CHUNKS):
            near[g][c].wait_recv()
        gather_step(g)

    half_copy = []
    for m in range(2):
        cxt = total[256 * m:256 * m + 256, :].astype(jnp.bfloat16)
        turned[m, :, 0:256] = mm(pick[m], cxt, NT).astype(jnp.bfloat16)
        for j in range(4):
            lo = 128 * j
            block = (mm(turned[m, lo:lo + 128, 0:256], turned[m, lo:, 256:512], NT)
                     + mm(turned[m, lo:lo + 128, 256:512], turned[m, lo:, 0:256], NT))
            for i in range(16):
                for row, col, lane, width in folded(i):
                    if lo <= row < lo + 128:
                        part[m, i % 2, i // 2, :, lane:lane + width] = block[row - lo:row - lo + 16, col - lo:]
        copy = send(part.at[m, 1 - k], half.at[m], sum_sem, m, sibling)
        copy.start()
        half_copy.append(copy)
    sums = [[], []]
    for m in range(2):
        half_copy[m].wait_recv()
        mine[m] = part[m, k] + half[m]
        for n, (dy, dz) in enumerate(others):
            yy, zz = chip_at(dy, dz)
            copy = send(mine.at[m, 2 * yy + zz], came.at[m, n], sum_sem, 2 + 7 * m + n, at(yy, zz, k))
            copy.start()
            sums[m].append(copy)
    both = []
    for m in range(2):
        whole = mine[m, chip]
        for n in range(7):
            sums[m][n].wait_recv()
            whole = whole + came[m, n]
        both.append(whole)

    lane = lax.broadcasted_iota(jnp.int32, (16, FOLD), 1)
    line = lax.broadcasted_iota(jnp.int32, (16, FOLD), 0)
    a = lax.div(me, 8)
    cut = ORDER - 128 * a
    low_part = lane < cut
    row = jnp.where(low_part, 16 * me, 16 * (31 - me)) + line
    col = jnp.where(low_part, 128 * a + lane, 128 * (3 - a) + lane - cut)
    order = orders[group]
    live = (row < order) & (col < order)
    formed[...] = jnp.where(live, both[0] * both[1], 0.0) + jnp.where(row == col, 1.0, 0.0)

    first = [send(formed, along.at[d - 1], x_sem, d - 1, {"blk": x_at(d)}) for d in (1, 2, 3)]
    for copy in first:
        copy.start()
    have = [(group, formed[...])]
    for d in (1, 2, 3):
        first[d - 1].wait_recv()
        have.append((x_at(4 - d), along[d - 1]))

    def bound_for(to):
        kept = jnp.zeros((16, FOLD), jnp.float32)
        for source, value in have:
            kept = jnp.where(dest[source] == to, value, kept)
        return kept

    second = []
    for d in (2, 1, 3):
        bound[d - 1] = bound_for(h_at(d))
        copy = send(bound.at[d - 1], brought.at[d - 1], h_sem, d - 1, {"blk": h_at(d)})
        copy.start()
        second.append((d, copy))
    here = bound_for(group)
    for d, copy in second:
        copy.wait_recv()
        here = here + brought[d - 1]
    pieces[me] = here

    outs = [send(pieces.at[me], pieces.at[me], out_sem, 0, sibling)]
    for n, (dy, dz) in enumerate(others):
        yy, zz = chip_at(dy, dz)
        outs.append(send(pieces.at[me], pieces.at[me], out_sem, 1 + n, at(yy, zz, k)))
    for copy in outs:
        copy.start()
    passed = []
    for n, (dy, dz) in enumerate(others):
        yy, zz = chip_at(4 - dy, dz)
        source = 4 * yy + 2 * zz + k
        outs[1 + n].wait_recv()
        copy = send(pieces.at[source], pieces.at[source], out_sem, 8 + n, sibling)
        copy.start()
        passed.append(copy)
    outs[0].wait_recv()
    for copy in passed:
        copy.wait_recv()
    for i in range(16):
        for row, col, lane, width in folded(i):
            s_ref[row:row + 16, col:col + width] = pieces[i, :, lane:lane + width]

    own_copy.wait_send()
    for copies in (z_copy, u_copy, w_copy, p_own, near[1], near[2], near[3], near[4], half_copy, *sums, first,
                   [copy for _, copy in second], outs, passed):
        for copy in copies:
            copy.wait_send()


def schur_block(x, y, v, index, orders, dest):
    bf, f32 = jnp.bfloat16, jnp.float32
    vm, dma = pltpu.VMEM, pltpu.SemaphoreType.DMA
    return pl.pallas_call(
        pair_kernel,
        out_shape=jax.ShapeDtypeStruct((ORDER, ORDER), f32),
        in_specs=[pl.BlockSpec(memory_space=pl.ANY)] * 2 + [pl.BlockSpec(memory_space=vm)] * 2
        + [pl.BlockSpec(memory_space=pltpu.SMEM)] * 2,
        out_specs=pl.BlockSpec(memory_space=vm),
        scratch_shapes=[
            vm((2, 5, 512, 256), bf), vm((512, 2560), bf), vm((5, 512, RANK), bf),
            vm((512, RANK), f32), vm((2, ORDER, RANK), bf), vm((2, ORDER, 512), bf),
            vm((2, 2, 8, 16, FOLD), f32), vm((2, 8, 16, FOLD), f32), vm((2, 8, 16, FOLD), f32),
            vm((2, 7, 16, FOLD), f32), vm((16, FOLD), f32), vm((3, 16, FOLD), f32), vm((3, 16, FOLD), f32),
            vm((3, 16, FOLD), f32), vm((16, 16, FOLD), f32),
            dma((10,)), dma((2, 1)), dma((2, 4 * CHUNKS)), dma((2, 4 * CHUNKS)), dma((2, 16)),
            dma((2, 3)), dma((2, 3)), dma((2, 15)),
        ],
        compiler_params=pltpu.CompilerParams(collective_id=0, has_side_effects=True),
    )(x, y, v, index, orders, dest)


def lane_of(x, k):
    return jnp.broadcast_to(x[:, k:k + 1], (8, 128))


def sub_of(x, k):
    return jnp.broadcast_to(x[k:k + 1, :], x.shape)


def panel(work, lo, p, lanes, cols):
    wide = [lo + 128 * v for v in range(lanes)]
    top = lo + 8 * p
    rows = [work[pl.ds(top, 8), pl.ds(w, 128)] for w in wide]
    sub = lax.broadcasted_iota(jnp.int32, (8, 128), 0)
    if cols is None:
        cols = [lane_of(rows[0], 8 * p + b) for b in range(8)]
    ahead = None
    inv, coef, urow = [], [], []
    scale = jnp.zeros((8, 128), jnp.float32)
    if p < 15:
        nxt = work[pl.ds(top + 8, 8), pl.ds(lo, 128)]
        side = [lane_of(nxt, 8 * p + b) for b in range(8)]
        ahead = [lane_of(nxt, 8 * p + 8 + b) for b in range(8)]
    for k in range(8):
        r = lax.rsqrt(sub_of(cols[k], k))
        d = r * r
        c = cols[k] * r
        cs = {b: sub_of(cols[k], b) for b in range(k + 1, 8)}
        for b in range(k + 1, 8):
            cols[b] = cols[b] - (cols[k] * cs[b]) * d
        u = [sub_of(x, k) * r for x in rows]
        cm = jnp.where(sub > k, c, 0.0)
        rows = [x - cm * y for x, y in zip(rows, u)]
        scale = jnp.where(sub == k, r, scale)
        inv.append(r)
        coef.append({b: x * r for b, x in cs.items()})
        urow.append(u)
        if ahead is not None:
            e = side[k] * r
            for b in range(k + 1, 8):
                side[b] = side[b] - e * coef[k][b]
            ahead = [x - e * sub_of(e, b) for b, x in enumerate(ahead)]
            side[k] = e
    done = [x * scale for x in rows]
    for x, w in zip(done, wide):
        work[pl.ds(top, 8), pl.ds(w, 128)] = x
    for g in range(p + 1, 16):
        at = lo + 8 * g
        rest = [work[pl.ds(at, 8), pl.ds(w, 128)] for w in wide]
        if g == p + 1:
            cs = side
        else:
            cs = [lane_of(rest[0], 8 * p + b) for b in range(8)]
            for k in range(8):
                cs[k] = cs[k] * inv[k]
                for b in range(k + 1, 8):
                    cs[b] = cs[b] - cs[k] * coef[k][b]
        for k in range(8):
            rest = [x - cs[k] * y for x, y in zip(rest, urow[k])]
        for x, w in zip(rest, wide):
            work[pl.ds(at, 8), pl.ds(w, 128)] = x
    return ahead


def factor(work, low, n):
    blocks = n // 128
    for j in range(blocks):
        lo = 128 * j
        cols = None
        for p in range(16):
            cols = panel(work, lo, p, blocks - j, cols)
        tri = lax.broadcasted_iota(jnp.int32, (128, 128), 0) >= lax.broadcasted_iota(jnp.int32, (128, 128), 1)
        low[pl.ds(lo, 128), pl.ds(lo, 128)] = jnp.where(tri, work[pl.ds(lo, 128), pl.ds(lo, 128)].T, 0.0)
        for i in range(j + 1, blocks):
            low[pl.ds(128 * i, 128), pl.ds(lo, 128)] = work[pl.ds(lo, 128), pl.ds(128 * i, 128)].T
            low[pl.ds(lo, 128), pl.ds(128 * i, 128)] = jnp.zeros((128, 128), jnp.float32)
        for i in range(j + 1, blocks):
            w = n - 128 * i
            work[pl.ds(128 * i, 128), pl.ds(128 * i, w)] = work[pl.ds(128 * i, 128), pl.ds(128 * i, w)] - lax.dot_general(
                low[pl.ds(128 * i, 128), pl.ds(lo, 128)], work[pl.ds(lo, 128), pl.ds(128 * i, w)],
                (((1,), (0,)), ((), ())), preferred_element_type=jnp.float32, precision=lax.Precision.HIGHEST)


def chol_kernel(s_ref, own_ref, work, low):
    n, share = s_ref.shape[0], own_ref.shape[0]
    work[...] = s_ref[...]
    factor(work, low, n)
    own_ref[...] = low[pl.ds(pl.multiple_of(share * lax.axis_index("slab"), share), share), :]


def chol_rows(s, share):
    n = s.shape[0]
    return pl.pallas_call(
        chol_kernel,
        out_shape=jax.ShapeDtypeStruct((share, n), jnp.float32),
        in_specs=[pl.BlockSpec(memory_space=pltpu.VMEM)],
        out_specs=pl.BlockSpec(memory_space=pltpu.VMEM),
        scratch_shapes=[pltpu.VMEM((n, n), jnp.float32)] * 2,
    )(s)


def on_device(xinv, ymat, basis, pair_index, orders, dest):
    whole = schur_block(xinv[0], ymat[0], basis[0], pair_index[0], orders, dest)
    return chol_rows(whole, ORDER // lax.axis_size("slab"))[None]


def solution(mesh):
    return jax.shard_map(
        on_device,
        mesh=mesh,
        in_specs=(
            P("blk", None, "slab"),
            P("blk", None, "slab"),
            P("blk", "slab", None),
            P("blk", None, None),
            P(),
            P(),
        ),
        out_specs=P("blk", "slab", None),
        check_vma=False,
    )
```

```python
import jax
import jax.numpy as jnp
from jax import lax
from jax.experimental import pallas as pl
from jax.experimental.pallas import tpu as pltpu
from jax.sharding import PartitionSpec as P

MESH = pl.DeviceIdType.MESH
CHUNKS = 4
ROWS, RANK, ORDER, FOLD = 256, 1024, 512, 640
PIECE = ROWS // CHUNKS
NT = (((1,), (1,)), ((), ()))
NN = (((1,), (0,)), ((), ()))


def mm(a, b, dims):
    return lax.dot_general(a, b, dims, preferred_element_type=jnp.float32)


def folded(i):
    a = i // 8
    cut = ORDER - 128 * a
    return ((16 * i, 128 * a, 0, cut), (16 * (31 - i), 128 * (3 - a), cut, FOLD - cut))


def pair_kernel(x_hbm, y_hbm, own, index, orders, dest, s_ref, xin, xyt, held, total, pick, turned,
                part, half, mine, came, formed, along, bound, brought, pieces,
                load_sem, own_sem, far_sem, near_sem, sum_sem, x_sem, h_sem, out_sem):
    me = lax.axis_index("slab")
    y, z, k = lax.div(me, 4), lax.rem(lax.div(me, 2), 2), lax.rem(me, 2)
    chip = 2 * y + z
    group = lax.axis_index("blk")
    bx, bh = lax.div(group, 4), lax.rem(group, 4)
    up, down, across = lax.rem(y + 1, 4), lax.rem(y + 3, 4), 1 - z

    def at(yy, zz, kk):
        return {"slab": 4 * yy + 2 * zz + kk}

    sibling, beside = at(y, z, 1 - k), at(y, across, k)
    above, below, slant = at(up, z, k), at(down, z, k), at(down, across, k)
    opposite = at(lax.rem(y + 2, 4), z, k)
    others = [(dy, dz) for dy in range(4) for dz in range(2) if (dy, dz) != (0, 0)]

    def chip_at(dy, dz):
        return lax.rem(y + dy, 4), z + dz - 2 * z * dz

    def send(src, dst, sems, i, to):
        return pltpu.make_async_remote_copy(
            src_ref=src, dst_ref=dst, send_sem=sems.at[0, i], recv_sem=sems.at[1, i],
            device_id=to, device_id_type=MESH)

    def x_at(d):
        return 4 * lax.rem(bx + d, 4) + bh

    def h_at(d):
        return 4 * bx + lax.rem(bh + d, 4)

    w = jnp.where(y >= 2, z, across)
    groups = (chip, 2 * y + across, 2 * down + z, 2 * up + across, 2 * lax.rem(y + 2, 4) + w)
    loads = []
    for m, src in enumerate((x_hbm, y_hbm)):
        for g, c in enumerate(groups):
            copy = pltpu.make_async_copy(
                src.at[pl.ds(pl.multiple_of(512 * c, 512), 512), :], xin.at[m, g], load_sem.at[5 * m + g])
            copy.start()
            loads.append(copy)

    barrier = pltpu.get_barrier_semaphore()
    pl.semaphore_signal(barrier, inc=1, device_id=sibling, device_id_type=MESH)
    for dy, dz in others:
        yy, zz = chip_at(dy, dz)
        pl.semaphore_signal(barrier, inc=1, device_id=at(yy, zz, k), device_id_type=MESH)
    for d in (1, 2, 3):
        for to in (x_at(d), h_at(d)):
            pl.semaphore_signal(barrier, inc=1, device_id={"blk": to}, device_id_type=MESH)
    pl.semaphore_wait(barrier, 14)

    base = pl.multiple_of(ROWS * k, ROWS)

    def rows(c):
        return pl.ds(pl.multiple_of(base + PIECE * c, PIECE), PIECE)

    def bit(c):
        return pl.ds(PIECE * c, PIECE)

    own_copy = send(own, held.at[0, pl.ds(base, ROWS), :], own_sem, 0, sibling)
    own_copy.start()
    z_copy = [send(own.at[bit(c), :], held.at[1, rows(c), :], far_sem, c, beside) for c in range(CHUNKS)]
    u_copy = [send(own.at[bit(c), :], held.at[2, rows(c), :], far_sem, CHUNKS + c, above) for c in range(CHUNKS)]
    w_copy = [send(held.at[1, rows(c), :] if c < CHUNKS // 2 else own.at[bit(c), :], held.at[3, rows(c), :],
                   far_sem, 2 * CHUNKS + c, below if c < CHUNKS // 2 else slant) for c in range(CHUNKS)]
    p_own = [send(own.at[bit(c), :], held.at[4, rows(c), :], far_sem, 3 * CHUNKS + c, opposite)
             for c in range(CHUNKS)]
    p_held = [send(held.at[1, rows(c), :], held.at[4, rows(c), :], far_sem, 3 * CHUNKS + c, opposite)
              for c in range(CHUNKS)]
    near = {g: [send(held.at[g, rows(c), :], held.at[g, rows(c), :], near_sem, CHUNKS * (g - 1) + c, sibling)
                for c in range(CHUNKS)] for g in (1, 2, 3, 4)}
    for c in range(CHUNKS):
        z_copy[c].start()
        u_copy[c].start()
    for c in range(CHUNKS // 2, CHUNKS):
        w_copy[c].start()

    @pl.when(y < 2)
    def _():
        for c in range(CHUNKS):
            p_own[c].start()

    held[0, pl.ds(base, ROWS), :] = own[...]
    for m in range(2):
        wanted = jnp.broadcast_to(index[m:m + 1, :], (128, ORDER)).astype(jnp.float32).T
        for j in range(RANK // 128):
            lane = lax.broadcasted_iota(jnp.int32, (ORDER, 128), 1).astype(jnp.float32) + 128.0 * j
            pick[m, :, 128 * j:128 * j + 128] = jnp.where(wanted == lane, 1.0, 0.0).astype(jnp.bfloat16)
        turned[m, :, 256:512] = mm(pick[m], own[...], NT).astype(jnp.bfloat16)
    for copy in loads:
        copy.wait()
    for m in range(2):
        for g in range(5):
            xt = xin[m, g].T
            if g < 2:
                xt = xt * jnp.bfloat16(0.5)
            xyt[256 * m:256 * m + 256, 512 * g:512 * g + 512] = xt

    def gather_step(g, first=False):
        for j in range(RANK // 256):
            cols = slice(256 * j, 256 * j + 256)
            more = mm(xyt[:, 512 * g:512 * g + 512], held[g, :, cols], NN)
            total[:, cols] = more if first else total[:, cols] + more

    own_copy.wait_recv()
    gather_step(0, first=True)
    for c in range(CHUNKS):
        z_copy[c].wait_recv()
        if c < CHUNKS // 2:
            w_copy[c].start()

        @pl.when(y >= 2)
        def _():
            p_held[c].start()

        near[1][c].start()
    for c in range(CHUNKS):
        near[1][c].wait_recv()
    gather_step(1)
    for c in range(CHUNKS):
        u_copy[c].wait_recv()
        near[2][c].start()
    for c in range(CHUNKS):
        near[2][c].wait_recv()
    gather_step(2)
    for c in range(CHUNKS):
        w_copy[c].wait_recv()
        near[3][c].start()
        p_own[c].wait_recv()
        near[4][c].start()
    for g in (3, 4):
        for c in range(CHUNKS):
            near[g][c].wait_recv()
        gather_step(g)

    half_copy = []
    for m in range(2):
        cxt = total[256 * m:256 * m + 256, :].astype(jnp.bfloat16)
        turned[m, :, 0:256] = mm(pick[m], cxt, NT).astype(jnp.bfloat16)
        for j in range(4):
            lo = 128 * j
            block = (mm(turned[m, lo:lo + 128, 0:256], turned[m, lo:, 256:512], NT)
                     + mm(turned[m, lo:lo + 128, 256:512], turned[m, lo:, 0:256], NT))
            for i in range(16):
                for row, col, lane, width in folded(i):
                    if lo <= row < lo + 128:
                        part[m, i % 2, i // 2, :, lane:lane + width] = block[row - lo:row - lo + 16, col - lo:]
        copy = send(part.at[m, 1 - k], half.at[m], sum_sem, m, sibling)
        copy.start()
        half_copy.append(copy)
    sums = [[], []]
    for m in range(2):
        half_copy[m].wait_recv()
        mine[m] = part[m, k] + half[m]
        for n, (dy, dz) in enumerate(others):
            yy, zz = chip_at(dy, dz)
            copy = send(mine.at[m, 2 * yy + zz], came.at[m, n], sum_sem, 2 + 7 * m + n, at(yy, zz, k))
            copy.start()
            sums[m].append(copy)
    both = []
    for m in range(2):
        whole = mine[m, chip]
        for n in range(7):
            sums[m][n].wait_recv()
            whole = whole + came[m, n]
        both.append(whole)

    lane = lax.broadcasted_iota(jnp.int32, (16, FOLD), 1)
    line = lax.broadcasted_iota(jnp.int32, (16, FOLD), 0)
    a = lax.div(me, 8)
    cut = ORDER - 128 * a
    low_part = lane < cut
    row = jnp.where(low_part, 16 * me, 16 * (31 - me)) + line
    col = jnp.where(low_part, 128 * a + lane, 128 * (3 - a) + lane - cut)
    order = orders[group]
    live = (row < order) & (col < order)
    formed[...] = jnp.where(live, both[0] * both[1], 0.0) + jnp.where(row == col, 1.0, 0.0)

    first = [send(formed, along.at[d - 1], x_sem, d - 1, {"blk": x_at(d)}) for d in (1, 2, 3)]
    for copy in first:
        copy.start()
    have = [(group, formed[...])]
    for d in (1, 2, 3):
        first[d - 1].wait_recv()
        have.append((x_at(4 - d), along[d - 1]))

    def bound_for(to):
        kept = jnp.zeros((16, FOLD), jnp.float32)
        for source, value in have:
            kept = jnp.where(dest[source] == to, value, kept)
        return kept

    second = []
    for d in (2, 1, 3):
        bound[d - 1] = bound_for(h_at(d))
        copy = send(bound.at[d - 1], brought.at[d - 1], h_sem, d - 1, {"blk": h_at(d)})
        copy.start()
        second.append((d, copy))
    here = bound_for(group)
    for d, copy in second:
        copy.wait_recv()
        here = here + brought[d - 1]
    pieces[me] = here

    outs = [send(pieces.at[me], pieces.at[me], out_sem, 0, sibling)]
    for n, (dy, dz) in enumerate(others):
        yy, zz = chip_at(dy, dz)
        outs.append(send(pieces.at[me], pieces.at[me], out_sem, 1 + n, at(yy, zz, k)))
    for copy in outs:
        copy.start()
    passed = []
    for n, (dy, dz) in enumerate(others):
        yy, zz = chip_at(4 - dy, dz)
        source = 4 * yy + 2 * zz + k
        outs[1 + n].wait_recv()
        copy = send(pieces.at[source], pieces.at[source], out_sem, 8 + n, sibling)
        copy.start()
        passed.append(copy)
    outs[0].wait_recv()
    for copy in passed:
        copy.wait_recv()
    for i in range(16):
        for row, col, lane, width in folded(i):
            s_ref[row:row + 16, col:col + width] = pieces[i, :, lane:lane + width]

    own_copy.wait_send()
    for copies in (z_copy, u_copy, w_copy, p_own, near[1], near[2], near[3], near[4], half_copy, *sums, first,
                   [copy for _, copy in second], outs, passed):
        for copy in copies:
            copy.wait_send()


def schur_block(x, y, v, index, orders, dest):
    bf, f32 = jnp.bfloat16, jnp.float32
    vm, dma = pltpu.VMEM, pltpu.SemaphoreType.DMA
    return pl.pallas_call(
        pair_kernel,
        out_shape=jax.ShapeDtypeStruct((ORDER, ORDER), f32),
        in_specs=[pl.BlockSpec(memory_space=pl.ANY)] * 2 + [pl.BlockSpec(memory_space=vm)] * 2
        + [pl.BlockSpec(memory_space=pltpu.SMEM)] * 2,
        out_specs=pl.BlockSpec(memory_space=vm),
        scratch_shapes=[
            vm((2, 5, 512, 256), bf), vm((512, 2560), bf), vm((5, 512, RANK), bf),
            vm((512, RANK), f32), vm((2, ORDER, RANK), bf), vm((2, ORDER, 512), bf),
            vm((2, 2, 8, 16, FOLD), f32), vm((2, 8, 16, FOLD), f32), vm((2, 8, 16, FOLD), f32),
            vm((2, 7, 16, FOLD), f32), vm((16, FOLD), f32), vm((3, 16, FOLD), f32), vm((3, 16, FOLD), f32),
            vm((3, 16, FOLD), f32), vm((16, 16, FOLD), f32),
            dma((10,)), dma((2, 1)), dma((2, 4 * CHUNKS)), dma((2, 4 * CHUNKS)), dma((2, 16)),
            dma((2, 3)), dma((2, 3)), dma((2, 15)),
        ],
        compiler_params=pltpu.CompilerParams(collective_id=0, has_side_effects=True),
    )(x, y, v, index, orders, dest)


def lane_of(x, k):
    return jnp.broadcast_to(x[:, k:k + 1], (8, 128))


def sub_of(x, k):
    return jnp.broadcast_to(x[k:k + 1, :], x.shape)


def panel(work, lo, p, end, lanes, cols):
    wide = [lo + 128 * v for v in range(lanes)]
    top = lo + 8 * p
    rows = [work[pl.ds(top, 8), pl.ds(w, 128)] for w in wide]
    sub = lax.broadcasted_iota(jnp.int32, (8, 128), 0)
    if cols is None:
        cols = [lane_of(rows[0], 8 * p + b) for b in range(8)]
    ahead = None
    inv, coef, urow = [], [], []
    scale = jnp.zeros((8, 128), jnp.float32)
    if p + 1 < end:
        nxt = work[pl.ds(top + 8, 8), pl.ds(lo, 128)]
        side = [lane_of(nxt, 8 * p + b) for b in range(8)]
        ahead = [lane_of(nxt, 8 * p + 8 + b) for b in range(8)]
    for k in range(8):
        r = lax.rsqrt(sub_of(cols[k], k))
        d = r * r
        c = cols[k] * r
        cs = {b: sub_of(cols[k], b) for b in range(k + 1, 8)}
        for b in range(k + 1, 8):
            cols[b] = cols[b] - (cols[k] * cs[b]) * d
        u = [sub_of(x, k) * r for x in rows]
        cm = jnp.where(sub > k, c, 0.0)
        rows = [x - cm * y for x, y in zip(rows, u)]
        scale = jnp.where(sub == k, r, scale)
        inv.append(r)
        coef.append({b: x * r for b, x in cs.items()})
        urow.append(u)
        if ahead is not None:
            e = side[k] * r
            for b in range(k + 1, 8):
                side[b] = side[b] - e * coef[k][b]
            ahead = [x - e * sub_of(e, b) for b, x in enumerate(ahead)]
            side[k] = e
    done = [x * scale for x in rows]
    for x, w in zip(done, wide):
        work[pl.ds(top, 8), pl.ds(w, 128)] = x
    for g in range(p + 1, end):
        at = lo + 8 * g
        rest = [work[pl.ds(at, 8), pl.ds(w, 128)] for w in wide]
        if g == p + 1:
            cs = side
        else:
            cs = [lane_of(rest[0], 8 * p + b) for b in range(8)]
            for k in range(8):
                cs[k] = cs[k] * inv[k]
                for b in range(k + 1, 8):
                    cs[b] = cs[b] - cs[k] * coef[k][b]
        for k in range(8):
            rest = [x - cs[k] * y for x, y in zip(rest, urow[k])]
        for x, w in zip(rest, wide):
            work[pl.ds(at, 8), pl.ds(w, 128)] = x
    return ahead


def factor(work, low, n):
    blocks = n // 128
    for j in range(blocks):
        lo = 128 * j
        cols = None
        for p in range(16):
            if p == 8:
                left = work[pl.ds(lo, 64), pl.ds(lo, 128)].T[64:, :]
                work[pl.ds(lo + 64, 64), pl.ds(lo, n - lo)] = work[pl.ds(lo + 64, 64), pl.ds(lo, n - lo)] - lax.dot_general(
                    left, work[pl.ds(lo, 64), pl.ds(lo, n - lo)], (((1,), (0,)), ((), ())),
                    preferred_element_type=jnp.float32, precision=lax.Precision.HIGHEST)
            cols = panel(work, lo, p, 8 if p < 8 else 16, blocks - j, cols)
        tri = lax.broadcasted_iota(jnp.int32, (128, 128), 0) >= lax.broadcasted_iota(jnp.int32, (128, 128), 1)
        low[pl.ds(lo, 128), pl.ds(lo, 128)] = jnp.where(tri, work[pl.ds(lo, 128), pl.ds(lo, 128)].T, 0.0)
        for i in range(j + 1, blocks):
            low[pl.ds(128 * i, 128), pl.ds(lo, 128)] = work[pl.ds(lo, 128), pl.ds(128 * i, 128)].T
            low[pl.ds(lo, 128), pl.ds(128 * i, 128)] = jnp.zeros((128, 128), jnp.float32)
        for i in range(j + 1, blocks):
            w = n - 128 * i
            work[pl.ds(128 * i, 128), pl.ds(128 * i, w)] = work[pl.ds(128 * i, 128), pl.ds(128 * i, w)] - lax.dot_general(
                low[pl.ds(128 * i, 128), pl.ds(lo, 128)], work[pl.ds(lo, 128), pl.ds(128 * i, w)],
                (((1,), (0,)), ((), ())), preferred_element_type=jnp.float32, precision=lax.Precision.HIGHEST)


def chol_kernel(s_ref, own_ref, work, low):
    n, share = s_ref.shape[0], own_ref.shape[0]
    work[...] = s_ref[...]
    factor(work, low, n)
    own_ref[...] = low[pl.ds(pl.multiple_of(share * lax.axis_index("slab"), share), share), :]


def chol_rows(s, share):
    n = s.shape[0]
    return pl.pallas_call(
        chol_kernel,
        out_shape=jax.ShapeDtypeStruct((share, n), jnp.float32),
        in_specs=[pl.BlockSpec(memory_space=pltpu.VMEM)],
        out_specs=pl.BlockSpec(memory_space=pltpu.VMEM),
        scratch_shapes=[pltpu.VMEM((n, n), jnp.float32)] * 2,
    )(s)


def on_device(xinv, ymat, basis, pair_index, orders, dest):
    whole = schur_block(xinv[0], ymat[0], basis[0], pair_index[0], orders, dest)
    return chol_rows(whole, ORDER // lax.axis_size("slab"))[None]


def solution(mesh):
    return jax.shard_map(
        on_device,
        mesh=mesh,
        in_specs=(
            P("blk", None, "slab"),
            P("blk", None, "slab"),
            P("blk", "slab", None),
            P("blk", None, None),
            P(),
            P(),
        ),
        out_specs=P("blk", "slab", None),
        check_vma=False,
    )
```

```python
import jax
import jax.numpy as jnp
from jax import lax
from jax.experimental import pallas as pl
from jax.experimental.pallas import tpu as pltpu
from jax.sharding import PartitionSpec as P

MESH = pl.DeviceIdType.MESH
CHUNKS = 4
ROWS, RANK, ORDER, FOLD = 256, 1024, 512, 640
PIECE = ROWS // CHUNKS
NT = (((1,), (1,)), ((), ()))
NN = (((1,), (0,)), ((), ()))


def mm(a, b, dims):
    return lax.dot_general(a, b, dims, preferred_element_type=jnp.float32)


def folded(i):
    a = i // 8
    cut = ORDER - 128 * a
    return ((16 * i, 128 * a, 0, cut), (16 * (31 - i), 128 * (3 - a), cut, FOLD - cut))


def pair_kernel(x_hbm, y_hbm, own, index, orders, dest, s_ref, xin, xyt, held, total, pick, turned,
                part, half, mine, came, formed, along, bound, brought, pieces,
                load_sem, own_sem, far_sem, near_sem, sum_sem, x_sem, h_sem, out_sem):
    me = lax.axis_index("slab")
    y, z, k = lax.div(me, 4), lax.rem(lax.div(me, 2), 2), lax.rem(me, 2)
    chip = 2 * y + z
    group = lax.axis_index("blk")
    bx, bh = lax.div(group, 4), lax.rem(group, 4)
    up, down, across = lax.rem(y + 1, 4), lax.rem(y + 3, 4), 1 - z

    def at(yy, zz, kk):
        return {"slab": 4 * yy + 2 * zz + kk}

    sibling, beside = at(y, z, 1 - k), at(y, across, k)
    above, below, slant = at(up, z, k), at(down, z, k), at(down, across, k)
    opposite = at(lax.rem(y + 2, 4), z, k)
    others = [(dy, dz) for dy in range(4) for dz in range(2) if (dy, dz) != (0, 0)]

    def chip_at(dy, dz):
        return lax.rem(y + dy, 4), z + dz - 2 * z * dz

    def send(src, dst, sems, i, to):
        return pltpu.make_async_remote_copy(
            src_ref=src, dst_ref=dst, send_sem=sems.at[0, i], recv_sem=sems.at[1, i],
            device_id=to, device_id_type=MESH)

    def x_at(d):
        return 4 * lax.rem(bx + d, 4) + bh

    def h_at(d):
        return 4 * bx + lax.rem(bh + d, 4)

    w = jnp.where(y >= 2, z, across)
    groups = (chip, 2 * y + across, 2 * down + z, 2 * up + across, 2 * lax.rem(y + 2, 4) + w)
    loads = []
    for m, src in enumerate((x_hbm, y_hbm)):
        for g, c in enumerate(groups):
            copy = pltpu.make_async_copy(
                src.at[pl.ds(pl.multiple_of(512 * c, 512), 512), :], xin.at[m, g], load_sem.at[5 * m + g])
            copy.start()
            loads.append(copy)

    barrier = pltpu.get_barrier_semaphore()
    pl.semaphore_signal(barrier, inc=1, device_id=sibling, device_id_type=MESH)
    for dy, dz in others:
        yy, zz = chip_at(dy, dz)
        pl.semaphore_signal(barrier, inc=1, device_id=at(yy, zz, k), device_id_type=MESH)
    for d in (1, 2, 3):
        for to in (x_at(d), h_at(d)):
            pl.semaphore_signal(barrier, inc=1, device_id={"blk": to}, device_id_type=MESH)
    pl.semaphore_wait(barrier, 14)

    base = pl.multiple_of(ROWS * k, ROWS)

    def rows(c):
        return pl.ds(pl.multiple_of(base + PIECE * c, PIECE), PIECE)

    def bit(c):
        return pl.ds(PIECE * c, PIECE)

    own_copy = send(own, held.at[0, pl.ds(base, ROWS), :], own_sem, 0, sibling)
    own_copy.start()
    z_copy = [send(own.at[bit(c), :], held.at[1, rows(c), :], far_sem, c, beside) for c in range(CHUNKS)]
    u_copy = [send(own.at[bit(c), :], held.at[2, rows(c), :], far_sem, CHUNKS + c, above) for c in range(CHUNKS)]
    w_copy = [send(held.at[1, rows(c), :] if c < CHUNKS // 2 else own.at[bit(c), :], held.at[3, rows(c), :],
                   far_sem, 2 * CHUNKS + c, below if c < CHUNKS // 2 else slant) for c in range(CHUNKS)]
    p_own = [send(own.at[bit(c), :], held.at[4, rows(c), :], far_sem, 3 * CHUNKS + c, opposite)
             for c in range(CHUNKS)]
    p_held = [send(held.at[1, rows(c), :], held.at[4, rows(c), :], far_sem, 3 * CHUNKS + c, opposite)
              for c in range(CHUNKS)]
    near = {g: [send(held.at[g, rows(c), :], held.at[g, rows(c), :], near_sem, CHUNKS * (g - 1) + c, sibling)
                for c in range(CHUNKS)] for g in (1, 2, 3, 4)}
    for c in range(CHUNKS):
        z_copy[c].start()
        u_copy[c].start()
    for c in range(CHUNKS // 2, CHUNKS):
        w_copy[c].start()

    @pl.when(y < 2)
    def _():
        for c in range(CHUNKS):
            p_own[c].start()

    held[0, pl.ds(base, ROWS), :] = own[...]
    for m in range(2):
        wanted = jnp.broadcast_to(index[m:m + 1, :], (128, ORDER)).astype(jnp.float32).T
        for j in range(RANK // 128):
            lane = lax.broadcasted_iota(jnp.int32, (ORDER, 128), 1).astype(jnp.float32) + 128.0 * j
            pick[m, :, 128 * j:128 * j + 128] = jnp.where(wanted == lane, 1.0, 0.0).astype(jnp.bfloat16)
        turned[m, :, 256:512] = mm(pick[m], own[...], NT).astype(jnp.bfloat16)
    for copy in loads:
        copy.wait()
    for m in range(2):
        for g in range(5):
            xt = xin[m, g].T
            if g < 2:
                xt = xt * jnp.bfloat16(0.5)
            xyt[256 * m:256 * m + 256, 512 * g:512 * g + 512] = xt

    def gather_step(g, first=False):
        for j in range(RANK // 256):
            cols = slice(256 * j, 256 * j + 256)
            more = mm(xyt[:, 512 * g:512 * g + 512], held[g, :, cols], NN)
            total[:, cols] = more if first else total[:, cols] + more

    own_copy.wait_recv()
    gather_step(0, first=True)
    for c in range(CHUNKS):
        z_copy[c].wait_recv()
        if c < CHUNKS // 2:
            w_copy[c].start()

        @pl.when(y >= 2)
        def _():
            p_held[c].start()

        near[1][c].start()
    for c in range(CHUNKS):
        near[1][c].wait_recv()
    gather_step(1)
    for c in range(CHUNKS):
        u_copy[c].wait_recv()
        near[2][c].start()
    for c in range(CHUNKS):
        near[2][c].wait_recv()
    gather_step(2)
    for c in range(CHUNKS):
        w_copy[c].wait_recv()
        near[3][c].start()
        p_own[c].wait_recv()
        near[4][c].start()
    for g in (3, 4):
        for c in range(CHUNKS):
            near[g][c].wait_recv()
        gather_step(g)

    half_copy = []
    for m in range(2):
        cxt = total[256 * m:256 * m + 256, :].astype(jnp.bfloat16)
        turned[m, :, 0:256] = mm(pick[m], cxt, NT).astype(jnp.bfloat16)
        for j in range(4):
            lo = 128 * j
            block = (mm(turned[m, lo:lo + 128, 0:256], turned[m, lo:, 256:512], NT)
                     + mm(turned[m, lo:lo + 128, 256:512], turned[m, lo:, 0:256], NT))
            for i in range(16):
                for row, col, lane, width in folded(i):
                    if lo <= row < lo + 128:
                        part[m, i % 2, i // 2, :, lane:lane + width] = block[row - lo:row - lo + 16, col - lo:]
        copy = send(part.at[m, 1 - k], half.at[m], sum_sem, m, sibling)
        copy.start()
        half_copy.append(copy)
    sums = [[], []]
    for m in range(2):
        half_copy[m].wait_recv()
        mine[m] = part[m, k] + half[m]
        for n, (dy, dz) in enumerate(others):
            yy, zz = chip_at(dy, dz)
            copy = send(mine.at[m, 2 * yy + zz], came.at[m, n], sum_sem, 2 + 7 * m + n, at(yy, zz, k))
            copy.start()
            sums[m].append(copy)
    both = []
    for m in range(2):
        whole = mine[m, chip]
        for n in range(7):
            sums[m][n].wait_recv()
            whole = whole + came[m, n]
        both.append(whole)

    lane = lax.broadcasted_iota(jnp.int32, (16, FOLD), 1)
    line = lax.broadcasted_iota(jnp.int32, (16, FOLD), 0)
    a = lax.div(me, 8)
    cut = ORDER - 128 * a
    low_part = lane < cut
    row = jnp.where(low_part, 16 * me, 16 * (31 - me)) + line
    col = jnp.where(low_part, 128 * a + lane, 128 * (3 - a) + lane - cut)
    order = orders[group]
    live = (row < order) & (col < order)
    value = jnp.where(live, both[0] * both[1], 0.0) + jnp.where(row == col, 1.0, 0.0)
    for q in range(2):
        formed[q] = value[8 * q:8 * q + 8, :]

    first = [[send(formed.at[q], along.at[q, d - 1], x_sem, 3 * q + d - 1, {"blk": x_at(d)}) for d in (1, 2, 3)]
             for q in range(2)]
    for copy in first[0] + first[1]:
        copy.start()
    second, here = [[], []], []
    for q in range(2):
        have = [(group, formed[q])]
        for d in (1, 2, 3):
            first[q][d - 1].wait_recv()
            have.append((x_at(4 - d), along[q, d - 1]))

        def bound_for(to):
            kept = jnp.zeros((8, FOLD), jnp.float32)
            for source, piece in have:
                kept = jnp.where(dest[source] == to, piece, kept)
            return kept

        for d in (2, 1, 3):
            bound[q, d - 1] = bound_for(h_at(d))
            copy = send(bound.at[q, d - 1], brought.at[q, d - 1], h_sem, 3 * q + d - 1, {"blk": h_at(d)})
            copy.start()
            second[q].append(copy)
        here.append(bound_for(group))

    outs = [[], []]
    for q in range(2):
        for n, d in enumerate((2, 1, 3)):
            second[q][n].wait_recv()
            here[q] = here[q] + brought[q, d - 1]
        pieces[q, me] = here[q]
        for n, (dy, dz) in enumerate(others):
            yy, zz = chip_at(dy, dz)
            outs[q].append(send(pieces.at[q, me], pieces.at[q, me], out_sem, 15 * q + n, at(yy, zz, k)))
        outs[q].append(send(pieces.at[q, me], pieces.at[q, me], out_sem, 15 * q + 7, sibling))
        for copy in outs[q]:
            copy.start()
    passed = []
    for q in range(2):
        for n, (dy, dz) in enumerate(others):
            yy, zz = chip_at(4 - dy, dz)
            source = 4 * yy + 2 * zz + k
            outs[q][n].wait_recv()
            copy = send(pieces.at[q, source], pieces.at[q, source], out_sem, 15 * q + 8 + n, sibling)
            copy.start()
            passed.append(copy)
    for q in range(2):
        outs[q][7].wait_recv()
    for copy in passed:
        copy.wait_recv()
    for i in range(16):
        for row, col, lane, width in folded(i):
            for q in range(2):
                s_ref[row + 8 * q:row + 8 * q + 8, col:col + width] = pieces[q, i, :, lane:lane + width]

    own_copy.wait_send()
    for copies in (z_copy, u_copy, w_copy, p_own, near[1], near[2], near[3], near[4], half_copy, *sums, *first,
                   *second, *outs, passed):
        for copy in copies:
            copy.wait_send()


def schur_block(x, y, v, index, orders, dest):
    bf, f32 = jnp.bfloat16, jnp.float32
    vm, dma = pltpu.VMEM, pltpu.SemaphoreType.DMA
    return pl.pallas_call(
        pair_kernel,
        out_shape=jax.ShapeDtypeStruct((ORDER, ORDER), f32),
        in_specs=[pl.BlockSpec(memory_space=pl.ANY)] * 2 + [pl.BlockSpec(memory_space=vm)] * 2
        + [pl.BlockSpec(memory_space=pltpu.SMEM)] * 2,
        out_specs=pl.BlockSpec(memory_space=vm),
        scratch_shapes=[
            vm((2, 5, 512, 256), bf), vm((512, 2560), bf), vm((5, 512, RANK), bf),
            vm((512, RANK), f32), vm((2, ORDER, RANK), bf), vm((2, ORDER, 512), bf),
            vm((2, 2, 8, 16, FOLD), f32), vm((2, 8, 16, FOLD), f32), vm((2, 8, 16, FOLD), f32),
            vm((2, 7, 16, FOLD), f32), vm((2, 8, FOLD), f32), vm((2, 3, 8, FOLD), f32), vm((2, 3, 8, FOLD), f32),
            vm((2, 3, 8, FOLD), f32), vm((2, 16, 8, FOLD), f32),
            dma((10,)), dma((2, 1)), dma((2, 4 * CHUNKS)), dma((2, 4 * CHUNKS)), dma((2, 16)),
            dma((2, 6)), dma((2, 6)), dma((2, 30)),
        ],
        compiler_params=pltpu.CompilerParams(collective_id=0, has_side_effects=True),
    )(x, y, v, index, orders, dest)


def lane_of(x, k):
    return jnp.broadcast_to(x[:, k:k + 1], (8, 128))


def sub_of(x, k):
    return jnp.broadcast_to(x[k:k + 1, :], x.shape)


def panel(work, lo, p, end, lanes, cols):
    wide = [lo + 128 * v for v in range(lanes)]
    top = lo + 8 * p
    rows = [work[pl.ds(top, 8), pl.ds(w, 128)] for w in wide]
    sub = lax.broadcasted_iota(jnp.int32, (8, 128), 0)
    if cols is None:
        cols = [lane_of(rows[0], 8 * p + b) for b in range(8)]
    ahead = None
    inv, coef, urow = [], [], []
    scale = jnp.zeros((8, 128), jnp.float32)
    if p + 1 < end:
        nxt = work[pl.ds(top + 8, 8), pl.ds(lo, 128)]
        side = [lane_of(nxt, 8 * p + b) for b in range(8)]
        ahead = [lane_of(nxt, 8 * p + 8 + b) for b in range(8)]
    for k in range(8):
        r = lax.rsqrt(sub_of(cols[k], k))
        d = r * r
        c = cols[k] * r
        cs = {b: sub_of(cols[k], b) for b in range(k + 1, 8)}
        for b in range(k + 1, 8):
            cols[b] = cols[b] - (cols[k] * cs[b]) * d
        u = [sub_of(x, k) * r for x in rows]
        cm = jnp.where(sub > k, c, 0.0)
        rows = [x - cm * y for x, y in zip(rows, u)]
        scale = jnp.where(sub == k, r, scale)
        inv.append(r)
        coef.append({b: x * r for b, x in cs.items()})
        urow.append(u)
        if ahead is not None:
            e = side[k] * r
            for b in range(k + 1, 8):
                side[b] = side[b] - e * coef[k][b]
            ahead = [x - e * sub_of(e, b) for b, x in enumerate(ahead)]
            side[k] = e
    done = [x * scale for x in rows]
    for x, w in zip(done, wide):
        work[pl.ds(top, 8), pl.ds(w, 128)] = x
    for g in range(p + 1, end):
        at = lo + 8 * g
        rest = [work[pl.ds(at, 8), pl.ds(w, 128)] for w in wide]
        if g == p + 1:
            cs = side
        else:
            cs = [lane_of(rest[0], 8 * p + b) for b in range(8)]
            for k in range(8):
                cs[k] = cs[k] * inv[k]
                for b in range(k + 1, 8):
                    cs[b] = cs[b] - cs[k] * coef[k][b]
        for k in range(8):
            rest = [x - cs[k] * y for x, y in zip(rest, urow[k])]
        for x, w in zip(rest, wide):
            work[pl.ds(at, 8), pl.ds(w, 128)] = x
    return ahead


def factor(work, low, n):
    blocks = n // 128
    for j in range(blocks):
        lo = 128 * j
        cols = None
        for p in range(16):
            if p == 8:
                left = work[pl.ds(lo, 64), pl.ds(lo, 128)].T[64:, :]
                work[pl.ds(lo + 64, 64), pl.ds(lo, n - lo)] = work[pl.ds(lo + 64, 64), pl.ds(lo, n - lo)] - lax.dot_general(
                    left, work[pl.ds(lo, 64), pl.ds(lo, n - lo)], (((1,), (0,)), ((), ())),
                    preferred_element_type=jnp.float32, precision=lax.Precision.HIGHEST)
            cols = panel(work, lo, p, 8 if p < 8 else 16, blocks - j, cols)
        tri = lax.broadcasted_iota(jnp.int32, (128, 128), 0) >= lax.broadcasted_iota(jnp.int32, (128, 128), 1)
        low[pl.ds(lo, 128), pl.ds(lo, 128)] = jnp.where(tri, work[pl.ds(lo, 128), pl.ds(lo, 128)].T, 0.0)
        for i in range(j + 1, blocks):
            low[pl.ds(128 * i, 128), pl.ds(lo, 128)] = work[pl.ds(lo, 128), pl.ds(128 * i, 128)].T
            low[pl.ds(lo, 128), pl.ds(128 * i, 128)] = jnp.zeros((128, 128), jnp.float32)
        for i in range(j + 1, blocks):
            w = n - 128 * i
            work[pl.ds(128 * i, 128), pl.ds(128 * i, w)] = work[pl.ds(128 * i, 128), pl.ds(128 * i, w)] - lax.dot_general(
                low[pl.ds(128 * i, 128), pl.ds(lo, 128)], work[pl.ds(lo, 128), pl.ds(128 * i, w)],
                (((1,), (0,)), ((), ())), preferred_element_type=jnp.float32, precision=lax.Precision.HIGHEST)


def chol_kernel(s_ref, own_ref, work, low):
    n, share = s_ref.shape[0], own_ref.shape[0]
    work[...] = s_ref[...]
    factor(work, low, n)
    own_ref[...] = low[pl.ds(pl.multiple_of(share * lax.axis_index("slab"), share), share), :]


def chol_rows(s, share):
    n = s.shape[0]
    return pl.pallas_call(
        chol_kernel,
        out_shape=jax.ShapeDtypeStruct((share, n), jnp.float32),
        in_specs=[pl.BlockSpec(memory_space=pltpu.VMEM)],
        out_specs=pl.BlockSpec(memory_space=pltpu.VMEM),
        scratch_shapes=[pltpu.VMEM((n, n), jnp.float32)] * 2,
    )(s)


def on_device(xinv, ymat, basis, pair_index, orders, dest):
    whole = schur_block(xinv[0], ymat[0], basis[0], pair_index[0], orders, dest)
    return chol_rows(whole, ORDER // lax.axis_size("slab"))[None]


def solution(mesh):
    return jax.shard_map(
        on_device,
        mesh=mesh,
        in_specs=(
            P("blk", None, "slab"),
            P("blk", None, "slab"),
            P("blk", "slab", None),
            P("blk", None, None),
            P(),
            P(),
        ),
        out_specs=P("blk", "slab", None),
        check_vma=False,
    )
```
